32 devices in a mesh: row: 4 (over y, x), col: 8 (over z, core).
Axes of the slice: x: 2, y: 2, z: 4, core: 2. Of those that a mesh axis runs over, the one named last changes fastest.
Arguments:
- factors: float32 [1, 8192, 8192], P(None, 'row', 'col'), may hold values from -20 to 30, as said below
Outputs:
- refreshed: float32 [1, 8192, 8192], P(None, 'row', 'col')
The draws below stay inside these ranges and needn't reach their ends.
Inputs may be any that keep to these rules, and one draw needn't show every extreme that they name: `factors`: every factor is symmetric positive definite.
All inputs are finite; a program needn't handle non-finite values.
Results may differ from the reference program's by a relative error of at most 0.0003.
Values sent between devices are 32-bit elements; how exact they have to be, the bound alone decides.
A program may use at most 64 MiB of HBM per device.

```python
import jax
import jax.numpy as jnp
from jax import lax

N = 8192
P_SIZE = 512
STEPS = 2
FACTORS = 1
N_COL = 8


def draw_factors(key, part):
    base_key = jax.random.fold_in(key, 11)
    position = jnp.arange(N, dtype=jnp.float32)
    rising = 3.0 ** (0.5 * position / N)
    scale_low, scale_high = (0.25, 0.75)

    def one_factor(member):
        noise_key, level_key, scale_key, shared_key = jax.random.split(jax.random.fold_in(base_key, member), 4)
        jitter = jax.random.normal(noise_key, (N, N), jnp.float32)
        shared = 0.5 * jax.random.truncated_normal(shared_key, -2.0, 2.0, (N, 8), jnp.float32)
        symmetric = (jitter + jitter.T) * (0.5 / jnp.sqrt(2.0 * N))
        common_part = jnp.dot(shared, shared.T, precision=lax.Precision.HIGHEST)
        levels = jax.random.uniform(level_key, (N,), jnp.float32, 2.0, 4.0)
        scales = jnp.exp(jax.random.uniform(scale_key, (N,), jnp.float32, jnp.log(scale_low), jnp.log(scale_high))) * rising
        matrix_core = symmetric + common_part + jnp.diag(levels)
        return scales[:, None] * matrix_core * scales[None, :]
    return lax.map(one_factor, jnp.arange(FACTORS))


def setup_inputs(seed: int = 0) -> dict:
    arg_keys = jax.random.split(jax.random.key(seed), 2)
    factors = draw_factors(jax.random.fold_in(arg_keys[1], 71), 0)
    return dict(factors=factors)


damping_share = 0.03162277660168379

def reference(factors):
    col_block = N // N_COL
    panel_slab = P_SIZE // N_COL
    sequence = jnp.arange(N, dtype=jnp.int32).reshape(N // col_block, col_block // panel_slab, panel_slab)
    sequence = sequence.transpose(1, 0, 2).reshape(N)
    restore = jnp.zeros((N,), jnp.int32).at[sequence].set(jnp.arange(N, dtype=jnp.int32))
    results = []
    for member in range(FACTORS):
        matrix = factors[member]
        damping = damping_share * jnp.trace(matrix) / N
        matrix = matrix + damping * jnp.eye(N, dtype=matrix.dtype)
        matrix = matrix[sequence][:, sequence]
        for section_no in range(STEPS):
            begin_at = section_no * P_SIZE
            finish = begin_at + P_SIZE
            factor_kk = jnp.linalg.cholesky(matrix[begin_at:finish, begin_at:finish])
            inverse_kk = jax.scipy.linalg.solve_triangular(factor_kk, jnp.eye(P_SIZE, dtype=matrix.dtype), lower=True)
            panel_rows = jnp.dot(matrix[finish:, begin_at:finish], inverse_kk.T, precision=lax.Precision.HIGHEST)
            update = jnp.dot(panel_rows, panel_rows.T, precision=lax.Precision.HIGHEST)
            matrix = matrix.at[finish:, finish:].add(-update)
            matrix = matrix.at[begin_at:finish, begin_at:finish].set(factor_kk)
            matrix = matrix.at[finish:, begin_at:finish].set(panel_rows)
            matrix = matrix.at[begin_at:finish, finish:].set(0.0)
        results.append(matrix[restore][:, restore])
    return jnp.stack(results)
```

```python
import functools

import jax
import jax.numpy as jnp
from jax import lax
from jax.experimental import pallas as pl
from jax.experimental.pallas import tpu as pltpu
from jax.sharding import PartitionSpec as P

P_SIZE = 512
STEPS = 2
TILE = 128

damping_share = 0.03162277660168379
top_precision = lax.Precision.HIGHEST
three_pass = lax.Precision.HIGH


def dot(a, b, dims, precision=top_precision):
    return lax.dot_general(
        a, b, (dims, ((), ())), precision=precision, preferred_element_type=jnp.float32
    )


def factor_tile(tile):
    size = tile.shape[0]
    groups = size // 8
    lane = lax.broadcasted_iota(jnp.int32, (8, size), 1)
    sub = lax.broadcasted_iota(jnp.int32, (8, size), 0)
    left = [tile[8 * t : 8 * t + 8, :] for t in range(groups)]
    right = [jnp.where(lane == sub + 8 * t, 1.0, 0.0).astype(jnp.float32) for t in range(groups)]

    def lanes(x, at):
        return jnp.broadcast_to(x[:, at : at + 1], x.shape)

    def rows(x, at):
        return jnp.broadcast_to(x[at : at + 1, :], x.shape)

    for j in range(groups):
        cols = [lanes(left[j], 8 * j + q) for q in range(8)]
        row_l, row_r = left[j], right[j]
        scales, coef, fin_l, fin_r = [], [], [], []
        out_l, out_r = row_l, row_r
        for i in range(8):
            pivot = rows(cols[i], i)
            s = lax.rsqrt(pivot)
            s = s * (1.5 - 0.5 * pivot * s * s)
            scales.append(s)
            l = cols[i] * s
            done_l = rows(row_l, i) * s
            done_r = rows(row_r, i) * s
            fin_l.append(done_l)
            fin_r.append(done_r)
            out_l = jnp.where(sub == i, done_l, out_l)
            out_r = jnp.where(sub == i, done_r, out_r)
            row_l = row_l - l * done_l
            row_r = row_r - l * done_r
            cq = {}
            for q in range(i + 1, 8):
                cq[q] = rows(l, q)
                cols[q] = cols[q] - l * cq[q]
            coef.append(cq)
        left[j] = jnp.where(lane >= sub + 8 * j, out_l, 0.0)
        right[j] = out_r
        for t in range(j + 1, groups):
            c = [lanes(left[t], 8 * j + q) for q in range(8)]
            acc_l, acc_r = left[t], right[t]
            for i in range(8):
                l = c[i] * scales[i]
                for q in range(i + 1, 8):
                    c[q] = c[q] - l * coef[i][q]
                acc_l = acc_l - l * fin_l[i]
                acc_r = acc_r - l * fin_r[i]
            left[t], right[t] = acc_l, acc_r
    return jnp.concatenate(left, axis=0), jnp.concatenate(right, axis=0)


def place_kernel(first_b, last_b, bpr, slab, order, at_ref, g_ref, s_ref, low_ref):
    total = STEPS * P_SIZE
    width = STEPS * slab
    per_tile = TILE // slab
    z_count, r_count = g_ref.shape[1], g_ref.shape[2]
    row_id, z_id, core = at_ref[0], at_ref[1], at_ref[2]

    def piece(r, c):
        z = lax.rem(c // 2 - z_id + z_count, z_count)
        return lax.rem(c + core, 2), z, jnp.bitwise_xor(r, row_id)

    def place(cp, carry):
        r, base = cp // bpr, (cp % bpr) * width
        for m in range(P_SIZE // TILE):
            where = [piece(r, m * per_tile + c) for c in range(per_tile)]
            for k in range(STEPS):
                got = [g_ref[i, j, l, pl.ds(base + k * slab, slab), :] for i, j, l in where]
                for kk in range(STEPS):
                    parts = [x[:, kk * slab : (kk + 1) * slab] for x in got]
                    s_ref[
                        pl.ds(pl.multiple_of(k * P_SIZE + cp * slab, 8), slab),
                        kk * P_SIZE + m * TILE : kk * P_SIZE + (m + 1) * TILE,
                    ] = jnp.concatenate(parts, axis=1)
        return carry

    lax.fori_loop(0, r_count * bpr, place, 0)
    trace = jnp.zeros((8, width), jnp.float32)
    for i in range(2):
        for j in range(z_count):
            for l in range(r_count):
                trace = trace + g_ref[i, j, l, bpr * width : bpr * width + 8, :]
    damping = damping_share * trace[0:1, 0:1] / order
    on_diag = lax.broadcasted_iota(jnp.int32, (TILE, TILE), 0) == lax.broadcasted_iota(
        jnp.int32, (TILE, TILE), 1
    )
    low_ref[...] = jnp.zeros_like(low_ref)

    def damp(b, carry):
        here = pl.ds(pl.multiple_of(b * TILE, TILE), TILE)
        tile = s_ref[here, here]
        s_ref[here, here] = tile + jnp.where(on_diag, jnp.broadcast_to(damping, tile.shape), 0.0)
        return carry

    lax.fori_loop(0, total // TILE, damp, 0)
    eliminate(first_b, last_b, s_ref, low_ref)


def eliminate(first_b, last_b, s_ref, low_ref):
    blocks = s_ref.shape[0] // TILE

    def step(b, carry):
        here = pl.ds(pl.multiple_of(b * TILE, TILE), TILE)
        upper, inverse = factor_tile(s_ref[here, here])
        low_ref[here, here] = upper.T
        s_ref[here, :] = dot(inverse, s_ref[here, :], ((1,), (0,)))
        s_ref[here, here] = inverse

        def trail(i, carry2):
            there = pl.ds(pl.multiple_of(i * TILE, TILE), TILE)
            low = dot(s_ref[there, here], inverse, ((1,), (1,)))
            low_ref[there, here] = low
            s_ref[there, here] = jnp.zeros((TILE, TILE), jnp.float32)
            s_ref[there, :] = s_ref[there, :] - dot(low, s_ref[here, :], ((1,), (0,)))
            return carry2

        lax.fori_loop(b + 1, blocks, trail, 0)
        return carry

    lax.fori_loop(first_b, last_b, step, 0)


def finish_kernel(
    whole, first_b, last_b, bpr, slab, col_count,
    at_ref, s_in, low_in, inv_ref, own_ref, s_ref, low_ref,
):
    total = STEPS * P_SIZE
    s_ref[...] = s_in[...]
    low_ref[...] = low_in[...]
    eliminate(first_b, last_b, s_ref, low_ref)

    def emit(i, carry):
        here = pl.ds(pl.multiple_of(i * TILE, TILE), TILE)
        value = s_ref[here, :]
        col = lax.broadcasted_iota(jnp.int32, value.shape, 1)
        value = jnp.where(col < (i + 1) * TILE, value, 0.0)
        if whole:
            inv_ref[here, :] = value
        else:
            for c in range(col_count):
                parts = [value[:, k * P_SIZE + c * slab :][:, :slab] for k in range(STEPS)]
                inv_ref[c, here, :] = jnp.concatenate(parts, axis=1)
        return carry

    lax.fori_loop(0, total // TILE, emit, 0)
    row_id = at_ref[0]
    col_id = at_ref[1] * 2 + at_ref[2]
    for c in range(col_count):

        @pl.when(col_id == c)
        def _():
            for b in range(bpr):
                for k in range(STEPS):
                    at = pl.multiple_of(k * P_SIZE + (row_id * bpr + b) * slab, 8)
                    value = low_ref[pl.ds(at, slab), :]
                    parts = [value[:, q * P_SIZE + c * slab :][:, :slab] for q in range(STEPS)]
                    own_ref[b, k * slab : (k + 1) * slab, :] = jnp.concatenate(parts, axis=1)


F32, BF16 = jnp.float32, jnp.bfloat16

def split(x):
    high = x.astype(BF16)
    return high, (x - high.astype(F32)).astype(BF16)


def mul(a, b):
    return lax.dot_general(a, b, (((1,), (0,)), ((), ())), preferred_element_type=F32)


def three(a_high, a_low, b_high, b_low):
    return mul(a_high, b_high) + mul(a_low, b_high) + mul(a_high, b_low)


MB = 256


def update_kernel(
    steps, slab, z_count, row_count, bpr, halves,
    at_ref, damp_ref, inv_ref, own_ref, factor_ref, *refs,
):
    col_count = 2 * z_count
    width = steps * slab
    total = width * col_count
    rows_dev, cols_dev = factor_ref.shape
    pieces, refs = refs[: len(halves)], refs[len(halves) :]
    row_pieces, refs = refs[:row_count], refs[row_count:]
    out_ref, a_ref, f_ref, pc_ref, ih, il, th, tl, xh, xl, yh, yl, rh, rl, in_sem, a_sem, f_sem, o_sem = refs
    row_id, z_id, core = at_ref[0], at_ref[1], at_ref[2]
    col_id = 2 * z_id + core
    tiles = rows_dev // MB
    blocks = total // MB

    def row_copies():
        for d in range(row_count):
            r = jnp.bitwise_xor(row_id, d)
            for b in range(bpr):
                for k in range(steps):
                    to = pl.multiple_of(k * (total // steps) + (r * bpr + b) * slab, slab)
                    yield pltpu.make_async_copy(
                        row_pieces[d].at[pl.ds(b * width + k * slab, slab), :],
                        pc_ref.at[pl.ds(to, slab), :],
                        in_sem,
                    )

    def a_copies(t):
        for ref, (j, first, count) in zip(pieces, halves):
            if first <= t * MB < first + count:
                yield pltpu.make_async_copy(
                    ref.at[pl.ds(t * MB - first, MB), :],
                    a_ref.at[pl.ds(t * MB, MB), pl.ds(j * width, width)],
                    a_sem.at[t],
                )

    def f_copy(t):
        at = pl.ds(t * MB, MB)
        return pltpu.make_async_copy(factor_ref.at[at, :], f_ref.at[at, :], f_sem.at[t])

    def out_copy(t):
        at = pl.ds(pl.multiple_of(t * MB, MB), MB)
        return pltpu.make_async_copy(f_ref.at[at, :], out_ref.at[at, :], o_sem.at[t])

    for copy in row_copies():
        copy.start()
    for t in range(tiles):
        for copy in a_copies(t):
            copy.start()
        f_copy(t).start()

    for b in range(blocks):
        for k in range(b + 1):
            here, there = pl.ds(b * MB, MB), pl.ds(k * MB, MB)
            value = inv_ref[here, there]
            ih[here, there], il[here, there] = split(value)
            th[there, here], tl[there, here] = split(value.T)

    pltpu.make_async_copy(pc_ref, pc_ref, in_sem).wait()

    def cut(i, carry):
        here = pl.ds(pl.multiple_of(i * 64, 64), 64)
        xh[here, :], xl[here, :] = split(pc_ref[here, :])
        return carry

    lax.fori_loop(0, total // 64, cut, 0)

    def forward(n, carry):
        cols = pl.ds(pl.multiple_of(n * MB, MB), MB)
        for b in range(blocks):
            here, k = pl.ds(b * MB, MB), pl.ds(0, (b + 1) * MB)
            value = three(ih[here, k], il[here, k], xh[k, cols], xl[k, cols])
            yh[here, cols], yl[here, cols] = split(value)
        return carry

    lax.fori_loop(0, cols_dev // MB, forward, 0)

    def place(sb):
        k, c = sb // col_count, sb % col_count
        z = lax.rem(c // 2 - z_id + z_count, z_count)
        side = jnp.bitwise_xor(c % 2, core)
        return pl.ds(pl.multiple_of((side * z_count + z) * width + k * slab, slab), slab)

    def back(n, carry):
        cols = pl.ds(pl.multiple_of(n * MB, MB), MB)
        for b in range(blocks):
            here, k = pl.ds(b * MB, MB), pl.ds(b * MB, total - b * MB)
            value = three(th[here, k], tl[here, k], yh[k, cols], yl[k, cols])
            high, low = split(value)
            for q in range(MB // slab):
                to = place(b * (MB // slab) + q)
                rh[to, cols] = high[q * slab : (q + 1) * slab, :]
                rl[to, cols] = low[q * slab : (q + 1) * slab, :]
        return carry

    lax.fori_loop(0, cols_dev // MB, back, 0)
    mine = [
        inv_ref[pl.ds(pl.multiple_of(k * (total // steps) + col_id * slab, slab), slab), :]
        for k in range(steps)
    ]
    mine = jnp.concatenate(mine, axis=0)
    for b in range(total // width):
        high, low = split(mine[:, b * width : (b + 1) * width].T)
        for q in range(width // slab):
            to = place(b * (width // slab) + q)
            rh[to, 0:width] = high[q * slab : (q + 1) * slab, :]
            rl[to, 0:width] = low[q * slab : (q + 1) * slab, :]

    damping = damp_ref[0]
    sub = lax.broadcasted_iota(jnp.int32, (MB, MB), 0)
    lane = lax.broadcasted_iota(jnp.int32, (MB, MB), 1)
    gap = lane - sub

    def tile(t, carry):
        here = pl.ds(pl.multiple_of(t * MB, MB), MB)
        pltpu.make_async_copy(a_ref.at[here, :], a_ref.at[here, :], a_sem.at[t]).wait()
        pltpu.make_async_copy(f_ref.at[here, :], f_ref.at[here, :], f_sem.at[t]).wait()
        a_high, a_low = split(a_ref[here, :])
        offset = row_id * rows_dev + t * MB - col_id * cols_dev
        for n in range(cols_dev // MB):
            cols = pl.ds(n * MB, MB)
            value = three(a_high, a_low, rh[:, cols], rl[:, cols])
            damped = f_ref[here, cols] + jnp.where(gap == offset - n * MB, damping, 0.0)
            left = damped - value
            if n == 0:
                left = jnp.where(lane < width, value, left)
            f_ref[here, cols] = left

        @pl.when(lax.rem(t, cols_dev // MB) == 0)
        def _():
            top = pl.ds(pl.multiple_of(t * MB, MB), width)
            f_ref[top, 0:width] = own_ref[t // (cols_dev // MB)]
            f_ref[top, width:] = jnp.zeros((width, cols_dev - width), F32)

        out_copy(t).start()
        return carry

    lax.fori_loop(0, tiles, tile, 0)
    for t in range(tiles):
        out_copy(t).wait()


def finish_update(at, damping, inv, own, factor, mine, other, row_pieces, steps, slab, z_count, row_count, bpr):
    total = inv.shape[0]
    rows_dev, cols_dev = factor.shape
    pieces, halves = [], []
    for j, piece in enumerate(mine + other):
        parts = piece if isinstance(piece, list) else [piece]
        first = 0
        for part in parts:
            pieces.append(part)
            halves.append((j, first, part.shape[0]))
            first += part.shape[0]
    smem, vmem, hbm = [pl.BlockSpec(memory_space=m) for m in (pltpu.SMEM, pltpu.VMEM, pl.ANY)]
    half = lambda: pltpu.VMEM((total, total), BF16)
    return pl.pallas_call(
        functools.partial(update_kernel, steps, slab, z_count, row_count, bpr, tuple(halves)),
        out_shape=jax.ShapeDtypeStruct(factor.shape, F32),
        in_specs=[smem, smem, vmem, vmem, hbm] + [hbm] * (len(pieces) + row_count),
        out_specs=hbm,
        scratch_shapes=[
            pltpu.VMEM(factor.shape, F32), pltpu.VMEM(factor.shape, F32), pltpu.VMEM((total, cols_dev), F32),
            half(), half(), half(), half(),
            pltpu.VMEM((total, cols_dev), BF16), pltpu.VMEM((total, cols_dev), BF16),
            pltpu.VMEM((total, cols_dev), BF16), pltpu.VMEM((total, cols_dev), BF16),
            pltpu.VMEM((total, cols_dev), BF16), pltpu.VMEM((total, cols_dev), BF16),
            pltpu.SemaphoreType.DMA, pltpu.SemaphoreType.DMA((rows_dev // MB,)),
            pltpu.SemaphoreType.DMA((rows_dev // MB,)), pltpu.SemaphoreType.DMA((rows_dev // MB,)),
        ],
        compiler_params=pltpu.CompilerParams(vmem_limit_bytes=56 * 1024 * 1024),
        cost_estimate=pl.CostEstimate(flops=20_000_000_000, bytes_accessed=32_000_000, transcendentals=0),
        name="update",
    )(at, damping, inv, own, factor, *pieces, *row_pieces)


def in_vmem(count):
    return [pl.BlockSpec(memory_space=pltpu.VMEM)] * count


in_smem = pl.BlockSpec(memory_space=pltpu.SMEM)


def cost(flops):
    return pl.CostEstimate(flops=flops, bytes_accessed=16_000_000, transcendentals=0)


def shift(x, hops):
    count = lax.axis_size("col")
    return lax.ppermute(x, "col", [(c, (c + 2 * hops) % count) for c in range(count)])


def sibling(x):
    count = lax.axis_size("col")
    return lax.ppermute(x, "col", [(c, c ^ 1) for c in range(count)])


def ring_first(x):
    return shift(x, 1), shift(x, -1), sibling(x)


def ring_rest(x, first, join=True):
    z_count = lax.axis_size("col") // 2
    left, right, near = first
    mine, other = [x] + [None] * (z_count - 1), [near] + [None] * (z_count - 1)
    middle = z_count // 2
    from_left, from_right = x, x
    for hop in range(1, middle):
        from_left = left if hop == 1 else shift(from_left, 1)
        from_right = right if hop == 1 else shift(from_right, -1)
        mine[z_count - hop], mine[hop] = from_left, from_right
        other[z_count - hop], other[hop] = sibling(from_left), sibling(from_right)
    half = x.shape[0] // 2
    top, bottom = shift(from_left[:half], 1), shift(from_right[half:], -1)
    mine[middle], other[middle] = [top, bottom], [sibling(top), sibling(bottom)]
    if join:
        mine[middle] = jnp.concatenate(mine[middle], axis=0)
        other[middle] = jnp.concatenate(other[middle], axis=0)
    return mine, other


def across_rows(x):
    count = lax.axis_size("row")
    return [x] + [
        lax.ppermute(x, "row", [(r, r ^ d) for r in range(count)]) for d in range(1, count)
    ]


def on_device(factors):
    members = factors.shape[0]
    return jnp.stack([one_factor(factors[m]) for m in range(members)])


def one_factor(factor):
    rows_dev, cols_dev = factor.shape
    col_count, row_count = lax.axis_size("col"), lax.axis_size("row")
    z_count = col_count // 2
    order = rows_dev * row_count
    row_id, col_id = lax.axis_index("row"), lax.axis_index("col")
    z_id, core = col_id // 2, col_id % 2
    bpr = rows_dev // cols_dev
    slab = P_SIZE // col_count
    width = STEPS * slab
    total = STEPS * P_SIZE
    blocks = total // TILE
    direct = width % 128 == 0 and rows_dev % (2 * MB) == 0 and cols_dev % MB == 0 and total == cols_dev
    row_global = row_id * rows_dev + jnp.arange(rows_dev, dtype=jnp.int32)
    col_global = col_id * cols_dev + jnp.arange(cols_dev, dtype=jnp.int32)
    on_diagonal = row_global[:, None] == col_global[None, :]
    local_trace = jnp.sum(jnp.where(on_diagonal, factor, 0.0))

    cols = factor[:, :width]
    rows = factor.reshape(bpr, cols_dev, cols_dev)[:, :width, :]
    diag = rows[:, :, :width].reshape(bpr * width, width)
    piece = jnp.concatenate([diag, jnp.full((8, width), local_trace)], axis=0)
    slabs = jnp.stack(across_rows(piece))
    mine, other = ring_rest(slabs, ring_first(slabs))
    gathered = jnp.stack([jnp.stack(mine), jnp.stack(other)])
    gathered, cols, rows = lax.optimization_barrier((gathered, cols, rows))

    first = ring_first(cols)
    row_pieces = across_rows(rows.reshape(bpr * width, cols_dev))
    at = jnp.stack([row_id, z_id, core]).astype(jnp.int32)
    square = jax.ShapeDtypeStruct((total, total), jnp.float32)
    params = pltpu.CompilerParams(vmem_limit_bytes=40 * 1024 * 1024)
    part, low = pl.pallas_call(
        functools.partial(place_kernel, 0, blocks // 2, bpr, slab, order),
        out_shape=(square, square),
        in_specs=[in_smem] + in_vmem(1),
        out_specs=tuple(in_vmem(2)),
        compiler_params=params,
        cost_estimate=cost(30_000_000_000),
    )(at, gathered)
    part, low, first = lax.optimization_barrier((part, low, first))
    mine, other = ring_rest(cols, first, not direct)
    inv, own = pl.pallas_call(
        functools.partial(finish_kernel, direct, blocks // 2, blocks, bpr, slab, col_count),
        out_shape=(
            square if direct else jax.ShapeDtypeStruct((col_count, total, width), jnp.float32),
            jax.ShapeDtypeStruct((bpr, width, width), jnp.float32),
        ),
        in_specs=[in_smem] + in_vmem(2),
        out_specs=tuple(in_vmem(2)),
        scratch_shapes=[pltpu.VMEM((total, total), jnp.float32)] * 2,
        compiler_params=params,
        cost_estimate=cost(25_000_000_000),
    )(at, part, low)
    damping = damping_share * jnp.sum(gathered[:, :, :, bpr * width, 0]) / order

    if direct:
        return finish_update(
            at, damping.reshape(1), inv, own, factor, mine, other, row_pieces,
            STEPS, slab, z_count, row_count, bpr,
        )

    inv_rows = [
        lax.dynamic_index_in_dim(inv, (row_id ^ d) * bpr + b, 0, keepdims=False)
        for d in range(row_count)
        for b in range(bpr)
    ]
    inv_cols = [
        lax.dynamic_index_in_dim(
            inv, (z_id + z) % z_count * 2 + (core ^ side), 0, keepdims=False
        )
        for side in range(2)
        for z in range(z_count)
    ]
    cross = dot(
        jnp.concatenate(inv_rows, axis=1), jnp.concatenate(row_pieces, axis=0), ((1,), (0,))
    )
    lower = dot(
        jnp.concatenate(mine + other, axis=1), jnp.concatenate(inv_cols, axis=1), ((1,), (1,))
    )
    update = dot(lower, cross, ((1,), (0,)), three_pass)

    lower5 = lower.reshape(rows_dev, STEPS, col_count, slab)
    new_cols = lax.dynamic_index_in_dim(lower5, col_id, 2, keepdims=False)
    new_cols = new_cols.reshape(bpr, cols_dev, width)
    new_cols = new_cols.at[:, :width, :].set(own).reshape(rows_dev, width)

    trailing = (row_global % cols_dev >= width)[:, None] & (col_global % cols_dev >= width)[None, :]
    working = factor + jnp.where(on_diagonal, damping, 0.0)
    out = jnp.where(trailing, working - update, 0.0)
    return out.at[:, :width].set(new_cols)


def solution(mesh):
    placed = (P(None, "row", "col"),)
    return jax.shard_map(
        on_device, mesh=mesh, in_specs=placed, out_specs=P(None, "row", "col"), check_vma=False
    )
```

```python
import functools

import jax
import jax.numpy as jnp
from jax import lax
from jax.experimental import pallas as pl
from jax.experimental.pallas import tpu as pltpu
from jax.sharding import PartitionSpec as P

P_SIZE = 512
STEPS = 2
TILE = 128

damping_share = 0.03162277660168379
top_precision = lax.Precision.HIGHEST
three_pass = lax.Precision.HIGH


def dot(a, b, dims, precision=top_precision):
    return lax.dot_general(
        a, b, (dims, ((), ())), precision=precision, preferred_element_type=jnp.float32
    )


def factor_tile(tile):
    size = tile.shape[0]
    groups = size // 8
    lane = lax.broadcasted_iota(jnp.int32, (8, size), 1)
    sub = lax.broadcasted_iota(jnp.int32, (8, size), 0)
    left = [tile[8 * t : 8 * t + 8, :] for t in range(groups)]
    right = [jnp.where(lane == sub + 8 * t, 1.0, 0.0).astype(jnp.float32) for t in range(groups)]

    def lanes(x, at):
        return jnp.broadcast_to(x[:, at : at + 1], x.shape)

    def rows(x, at):
        return jnp.broadcast_to(x[at : at + 1, :], x.shape)

    for j in range(groups):
        cols = [lanes(left[j], 8 * j + q) for q in range(8)]
        row_l, row_r = left[j], right[j]
        scales, coef, fin_l, fin_r = [], [], [], []
        out_l, out_r = row_l, row_r
        for i in range(8):
            pivot = rows(cols[i], i)
            s = lax.rsqrt(pivot)
            s = s * (1.5 - 0.5 * pivot * s * s)
            scales.append(s)
            l = cols[i] * s
            done_l = rows(row_l, i) * s
            done_r = rows(row_r, i) * s
            fin_l.append(done_l)
            fin_r.append(done_r)
            out_l = jnp.where(sub == i, done_l, out_l)
            out_r = jnp.where(sub == i, done_r, out_r)
            row_l = row_l - l * done_l
            row_r = row_r - l * done_r
            cq = {}
            for q in range(i + 1, 8):
                cq[q] = rows(l, q)
                cols[q] = cols[q] - l * cq[q]
            coef.append(cq)
        left[j] = jnp.where(lane >= sub + 8 * j, out_l, 0.0)
        right[j] = out_r
        for t in range(j + 1, groups):
            c = [lanes(left[t], 8 * j + q) for q in range(8)]
            acc_l, acc_r = left[t], right[t]
            for i in range(8):
                l = c[i] * scales[i]
                for q in range(i + 1, 8):
                    c[q] = c[q] - l * coef[i][q]
                acc_l = acc_l - l * fin_l[i]
                acc_r = acc_r - l * fin_r[i]
            left[t], right[t] = acc_l, acc_r
    return jnp.concatenate(left, axis=0), jnp.concatenate(right, axis=0)


def place_kernel(first_b, last_b, bpr, slab, order, at_ref, g_ref, s_ref, low_ref):
    total = STEPS * P_SIZE
    width = STEPS * slab
    per_tile = TILE // slab
    z_count, r_count = g_ref.shape[1], g_ref.shape[2]
    row_id, z_id, core = at_ref[0], at_ref[1], at_ref[2]

    def piece(r, c):
        z = lax.rem(c // 2 - z_id + z_count, z_count)
        return lax.rem(c + core, 2), z, jnp.bitwise_xor(r, row_id)

    def place(cp, carry):
        r, base = cp // bpr, (cp % bpr) * width
        for m in range(P_SIZE // TILE):
            where = [piece(r, m * per_tile + c) for c in range(per_tile)]
            for k in range(STEPS):
                got = [g_ref[i, j, l, pl.ds(base + k * slab, slab), :] for i, j, l in where]
                for kk in range(STEPS):
                    parts = [x[:, kk * slab : (kk + 1) * slab] for x in got]
                    s_ref[
                        pl.ds(pl.multiple_of(k * P_SIZE + cp * slab, 8), slab),
                        kk * P_SIZE + m * TILE : kk * P_SIZE + (m + 1) * TILE,
                    ] = jnp.concatenate(parts, axis=1)
        return carry

    lax.fori_loop(0, r_count * bpr, place, 0)
    trace = jnp.zeros((8, width), jnp.float32)
    for i in range(2):
        for j in range(z_count):
            for l in range(r_count):
                trace = trace + g_ref[i, j, l, bpr * width : bpr * width + 8, :]
    damping = damping_share * trace[0:1, 0:1] / order
    on_diag = lax.broadcasted_iota(jnp.int32, (TILE, TILE), 0) == lax.broadcasted_iota(
        jnp.int32, (TILE, TILE), 1
    )
    low_ref[...] = jnp.zeros_like(low_ref)

    def damp(b, carry):
        here = pl.ds(pl.multiple_of(b * TILE, TILE), TILE)
        tile = s_ref[here, here]
        s_ref[here, here] = tile + jnp.where(on_diag, jnp.broadcast_to(damping, tile.shape), 0.0)
        return carry

    lax.fori_loop(0, total // TILE, damp, 0)
    eliminate(first_b, last_b, s_ref, low_ref)


def eliminate(first_b, last_b, s_ref, low_ref):
    blocks = s_ref.shape[0] // TILE

    def step(b, carry):
        here = pl.ds(pl.multiple_of(b * TILE, TILE), TILE)
        upper, inverse = factor_tile(s_ref[here, here])
        low_ref[here, here] = upper.T
        s_ref[here, :] = dot(inverse, s_ref[here, :], ((1,), (0,)))
        s_ref[here, here] = inverse

        def trail(i, carry2):
            there = pl.ds(pl.multiple_of(i * TILE, TILE), TILE)
            low = dot(s_ref[there, here], inverse, ((1,), (1,)))
            low_ref[there, here] = low
            s_ref[there, here] = jnp.zeros((TILE, TILE), jnp.float32)
            s_ref[there, :] = s_ref[there, :] - dot(low, s_ref[here, :], ((1,), (0,)))
            return carry2

        lax.fori_loop(b + 1, blocks, trail, 0)
        return carry

    lax.fori_loop(first_b, last_b, step, 0)


def finish_kernel(
    first_b, last_b, bpr, slab, col_count,
    at_ref, s_in, low_in, inv_ref, own_ref, s_ref, low_ref,
):
    total = STEPS * P_SIZE
    s_ref[...] = s_in[...]
    low_ref[...] = low_in[...]
    eliminate(first_b, last_b, s_ref, low_ref)

    def emit(i, carry):
        here = pl.ds(pl.multiple_of(i * TILE, TILE), TILE)
        value = s_ref[here, :]
        col = lax.broadcasted_iota(jnp.int32, value.shape, 1)
        value = jnp.where(col < (i + 1) * TILE, value, 0.0)
        for c in range(col_count):
            parts = [value[:, k * P_SIZE + c * slab :][:, :slab] for k in range(STEPS)]
            inv_ref[c, here, :] = jnp.concatenate(parts, axis=1)
        return carry

    lax.fori_loop(0, total // TILE, emit, 0)
    row_id = at_ref[0]
    col_id = at_ref[1] * 2 + at_ref[2]
    for c in range(col_count):

        @pl.when(col_id == c)
        def _():
            for b in range(bpr):
                for k in range(STEPS):
                    at = pl.multiple_of(k * P_SIZE + (row_id * bpr + b) * slab, 8)
                    value = low_ref[pl.ds(at, slab), :]
                    parts = [value[:, q * P_SIZE + c * slab :][:, :slab] for q in range(STEPS)]
                    own_ref[b, k * slab : (k + 1) * slab, :] = jnp.concatenate(parts, axis=1)


F32, BF16 = jnp.float32, jnp.bfloat16

def split(x):
    high = x.astype(BF16)
    return high, (x - high.astype(F32)).astype(BF16)


def mul(a, b):
    return lax.dot_general(a, b, (((1,), (0,)), ((), ())), preferred_element_type=F32)


def three(a_high, a_low, b_high, b_low):
    return mul(a_high, b_high) + mul(a_low, b_high) + mul(a_high, b_low)


MB = 256


def update_kernel(
    steps, slab, z_count, row_count, bpr,
    damp_ref, inv_ref, own_ref, factor_ref, ar_ref, ap_ref,
    out_ref, a_ref, f_ref, pc_ref, ih, il, th, tl, xh, xl, yh, yl, rh, rl, in_sem, a_sem, f_sem, o_sem,
):
    col_count = 2 * z_count
    width = steps * slab
    total = width * col_count
    cols_dev = factor_ref.shape[2]
    rows_dev = bpr * cols_dev
    row_id, col_id = lax.axis_index("row"), lax.axis_index("col")
    z_id, core = col_id // 2, lax.rem(col_id, 2)
    tiles = rows_dev // MB
    per = cols_dev // MB
    rest = pl.ds(width, cols_dev - width)
    blocks = total // MB

    def piece_copies():
        for d in range(row_count):
            r = jnp.bitwise_xor(row_id, d)
            for b in range(bpr):
                for k in range(steps):
                    to = pl.multiple_of(k * (total // steps) + (r * bpr + b) * slab, slab)
                    at = pl.ds(k * slab, slab)
                    source = factor_ref.at[b, at, rest] if d == 0 else ap_ref.at[r, b, at, rest]
                    yield pltpu.make_async_copy(source, pc_ref.at[pl.ds(to, slab), rest], in_sem)

    def a_copies(t):
        b, first = t // per, (t % per) * MB
        skip = width if first == 0 else 0
        at = pl.ds(first + skip, MB - skip)
        for j in range(col_count):
            c = lax.rem(z_id + j % z_count, z_count) * 2 + jnp.bitwise_xor(core, j // z_count)
            source = factor_ref.at[b, at, 0:width] if j == 0 else ar_ref.at[c, b, at, :]
            yield pltpu.make_async_copy(
                source, a_ref.at[pl.ds(t * MB + skip, MB - skip), pl.ds(j * width, width)], a_sem.at[t]
            )

    def f_copy(t, sem):
        return pltpu.make_async_copy(
            factor_ref.at[t // per, pl.ds((t % per) * MB, MB), :], f_ref.at[pl.ds(t * MB, MB), :], f_sem.at[sem]
        )

    def out_copy(t):
        at = pl.ds(pl.multiple_of(t * MB, MB), MB)
        return pltpu.make_async_copy(f_ref.at[at, :], out_ref.at[at, :], o_sem.at[t])

    for copy in piece_copies():
        copy.start()
    for t in range(tiles):
        for copy in a_copies(t):
            copy.start()
        f_copy(t, t).start()
    pc_ref[:, 0:width] = jnp.zeros((total, width), F32)
    for b in range(bpr):
        a_ref[b * cols_dev : b * cols_dev + width, :] = jnp.zeros((width, total), F32)

    for b in range(blocks):
        for k in range(b + 1):
            here, there = pl.ds(b * MB, MB), pl.ds(k * MB, MB)
            value = inv_ref[here, there]
            ih[here, there], il[here, there] = split(value)
            th[there, here], tl[there, here] = split(value.T)

    pltpu.make_async_copy(pc_ref.at[:, rest], pc_ref.at[:, rest], in_sem).wait()

    def cut(i, carry):
        here = pl.ds(pl.multiple_of(i * 64, 64), 64)
        xh[here, :], xl[here, :] = split(pc_ref[here, :])
        return carry

    lax.fori_loop(0, total // 64, cut, 0)

    def forward(n, carry):
        cols = pl.ds(pl.multiple_of(n * MB, MB), MB)
        for b in range(blocks):
            here, k = pl.ds(b * MB, MB), pl.ds(0, (b + 1) * MB)
            value = three(ih[here, k], il[here, k], xh[k, cols], xl[k, cols])
            yh[here, cols], yl[here, cols] = split(value)
        return carry

    lax.fori_loop(0, cols_dev // MB, forward, 0)

    def place(sb):
        k, c = sb // col_count, sb % col_count
        z = lax.rem(c // 2 - z_id + z_count, z_count)
        side = jnp.bitwise_xor(c % 2, core)
        return pl.ds(pl.multiple_of((side * z_count + z) * width + k * slab, slab), slab)

    def back(n, carry):
        cols = pl.ds(pl.multiple_of(n * MB, MB), MB)
        for b in range(blocks):
            here, k = pl.ds(b * MB, MB), pl.ds(b * MB, total - b * MB)
            value = three(th[here, k], tl[here, k], yh[k, cols], yl[k, cols])
            high, low = split(value)
            for q in range(MB // slab):
                to = place(b * (MB // slab) + q)
                rh[to, cols] = high[q * slab : (q + 1) * slab, :]
                rl[to, cols] = low[q * slab : (q + 1) * slab, :]
        return carry

    lax.fori_loop(0, cols_dev // MB, back, 0)
    mine = [
        inv_ref[pl.ds(pl.multiple_of(k * (total // steps) + col_id * slab, slab), slab), :]
        for k in range(steps)
    ]
    mine = jnp.concatenate(mine, axis=0)
    for b in range(total // width):
        high, low = split(mine[:, b * width : (b + 1) * width].T)
        for q in range(width // slab):
            to = place(b * (width // slab) + q)
            rh[to, 0:width] = high[q * slab : (q + 1) * slab, :]
            rl[to, 0:width] = low[q * slab : (q + 1) * slab, :]

    damping = damp_ref[0:1, 0:1]
    for t in range(tiles):
        skip = width if t % per == 0 else 0
        filled = a_ref.at[pl.ds(t * MB + skip, MB - skip), :]
        pltpu.make_async_copy(filled, filled, a_sem.at[t]).wait()
    sub = lax.broadcasted_iota(jnp.int32, (MB, MB), 0)
    lane = lax.broadcasted_iota(jnp.int32, (MB, MB), 1)
    gap = lane - sub

    def tile(t, carry):
        here = pl.ds(pl.multiple_of(t * MB, MB), MB)
        f_copy(0, t).wait()
        a_high, a_low = split(a_ref[here, :])
        offset = row_id * rows_dev + t * MB - col_id * cols_dev
        for n in range(cols_dev // MB):
            cols = pl.ds(n * MB, MB)
            value = three(a_high, a_low, rh[:, cols], rl[:, cols])
            damped = f_ref[here, cols] + jnp.where(gap == offset - n * MB, jnp.broadcast_to(damping, gap.shape), 0.0)
            left = damped - value
            if n == 0:
                left = jnp.where(lane < width, value, left)
            f_ref[here, cols] = left

        @pl.when(lax.rem(t, cols_dev // MB) == 0)
        def _():
            top = pl.ds(pl.multiple_of(t * MB, MB), width)
            f_ref[top, 0:width] = own_ref[t // (cols_dev // MB)]
            f_ref[top, width:] = jnp.zeros((width, cols_dev - width), F32)

        out_copy(t).start()
        return carry

    lax.fori_loop(0, tiles, tile, 0)
    for t in range(tiles):
        out_copy(t).wait()


def finish_update(damping, inv, own, factor3, ar, ap, slab, z_count, row_count):
    total = inv.shape[0]
    bpr, cols_dev = factor3.shape[0], factor3.shape[1]
    rows_dev = bpr * cols_dev
    vmem, hbm = [pl.BlockSpec(memory_space=m) for m in (pltpu.VMEM, pl.ANY)]
    tiles = rows_dev // MB
    return pl.pallas_call(
        functools.partial(update_kernel, STEPS, slab, z_count, row_count, bpr),
        out_shape=jax.ShapeDtypeStruct((rows_dev, cols_dev), F32),
        in_specs=[vmem, vmem, vmem, hbm, hbm, hbm],
        out_specs=hbm,
        scratch_shapes=[pltpu.VMEM((rows_dev, total), F32), pltpu.VMEM((rows_dev, cols_dev), F32)]
        + [pltpu.VMEM((total, cols_dev), F32)]
        + [pltpu.VMEM((total, total), BF16)] * 4
        + [pltpu.VMEM((total, cols_dev), BF16)] * 6
        + [pltpu.SemaphoreType.DMA]
        + [pltpu.SemaphoreType.DMA((tiles,))] * 3,
        compiler_params=pltpu.CompilerParams(vmem_limit_bytes=56 * 1024 * 1024),
        cost_estimate=pl.CostEstimate(flops=20_000_000_000, bytes_accessed=32_000_000, transcendentals=0),
        name="update",
    )(damping, inv, own, factor3, ar, ap)


def lane_copies(x, at):
    return jnp.broadcast_to(x[:, at : at + 1], x.shape)


def row_copies(x, at):
    return jnp.broadcast_to(x[at : at + 1, :], x.shape)


def factor_small(tile):
    groups = tile.shape[0] // 8
    sub = lax.broadcasted_iota(jnp.int32, (8, tile.shape[1]), 0)
    g = [tile[8 * t : 8 * t + 8, :] for t in range(groups)]
    cols = [lane_copies(g[0], q) for q in range(8)]
    for j in range(groups):
        row = out = g[j]
        scales, coef, fin = [], [], []
        more = j + 1 < groups
        if more:
            near = [lane_copies(g[j + 1], 8 * j + q) for q in range(8)]
            after = [lane_copies(g[j + 1], 8 * j + 8 + q) for q in range(8)]
            acc = g[j + 1]
        for i in range(8):
            s = lax.rsqrt(row_copies(cols[i], i))
            l = cols[i] * s
            cq = {q: row_copies(l, q) for q in range(i + 1, 8)}
            for q in range(i + 1, 8):
                cols[q] = cols[q] - l * cq[q]
            done = row_copies(row, i) * s
            out = jnp.where(sub == i, done, out)
            row = row - l * done
            scales.append(s)
            coef.append(cq)
            fin.append(done)
            if more:
                l = near[i] * s
                for q in range(i + 1, 8):
                    near[q] = near[q] - l * cq[q]
                for q in range(8):
                    after[q] = after[q] - l * row_copies(l, q)
                acc = acc - l * done
        g[j] = out
        if more:
            g[j + 1], cols = acc, after
        for t in range(j + 2, groups):
            c = [lane_copies(g[t], 8 * j + q) for q in range(8)]
            acc = g[t]
            for i in range(8):
                l = c[i] * scales[i]
                for q in range(i + 1, 8):
                    c[q] = c[q] - l * coef[i][q]
                acc = acc - l * fin[i]
            g[t] = acc
    lane = lax.broadcasted_iota(jnp.int32, tile.shape, 1)
    height = lax.broadcasted_iota(jnp.int32, tile.shape, 0)
    return jnp.where(lane >= height, jnp.concatenate(g, axis=0), 0.0)


def dot3(a, b):
    return three(*split(a), *split(b))


def factor_block(block):
    half = TILE // 2
    eye = jnp.where(
        lax.broadcasted_iota(jnp.int32, (half, half), 0) == lax.broadcasted_iota(jnp.int32, (half, half), 1), 1.0, 0.0
    ).astype(F32)
    first = factor_small(jnp.concatenate([block[:half, :half], eye], axis=1))
    u1, i1 = first[:, :half], first[:, half:]
    cross = dot3(i1, block[:half, half:])
    low = cross.T
    second = factor_small(jnp.concatenate([block[half:, half:] - dot3(low, cross), eye], axis=1))
    u2, i2 = second[:, :half], second[:, half:]
    i21 = -dot3(i2, dot3(low, i1))
    none = jnp.zeros((half, half), F32)
    upper = jnp.concatenate(
        [jnp.concatenate([u1, cross], axis=1), jnp.concatenate([none, u2], axis=1)], axis=0
    )
    inverse = jnp.concatenate(
        [jnp.concatenate([i1, none], axis=1), jnp.concatenate([i21, i2], axis=1)], axis=0
    )
    return upper, inverse


def at_block(b):
    return pl.ds(pl.multiple_of(b * TILE, TILE), TILE)


def eliminate_block(b, per_half, s_ref, up_ref, rh, rl):
    here = at_block(b)
    upper, inverse = factor_block(s_ref[here, here])
    total = s_ref.shape[1]
    ih, il = split(inverse)
    for n in range(0, total, 256):
        cols = pl.ds(n, 256)
        value = three(ih, il, *split(s_ref[here, cols]))
        done = lax.broadcasted_iota(jnp.int32, value.shape, 1) < (b + 1) * TILE - n
        s_ref[here, cols] = jnp.where(done, value, 0.0)
        up_ref[here, cols] = jnp.where(done, 0.0, value)
        rh[:, cols], rl[:, cols] = split(value)
    up_ref[here, here] = upper
    s_ref[here, here] = inverse

    def trail(t, carry):
        there = at_block(t)
        low_h, low_l = split(up_ref[here, there].T)
        for n in range(0, total, 256):
            cols = pl.ds(n, 256)
            s_ref[there, cols] = s_ref[there, cols] - three(low_h, low_l, rh[:, cols], rl[:, cols])
        s_ref[there, here] = -three(low_h, low_l, ih, il)
        return carry

    lax.fori_loop(b + 1, (b // per_half + 1) * per_half, trail, 0)


def second_half(s_ref, up_ref):
    half = s_ref.shape[0] // 2
    for i in range(half // 256):
        rows = pl.ds(half + i * 256, 256)
        low_h, low_l = split(up_ref[0:half, rows].T)
        for n in range(half // 256):
            left, right = pl.ds(n * 256, 256), pl.ds(half + n * 256, 256)
            x = s_ref[n * 256 : half, left]
            s_ref[rows, left] = -three(low_h[:, n * 256 :], low_l[:, n * 256 :], *split(x))
            u = up_ref[0:half, right]
            s_ref[rows, right] = s_ref[rows, right] - three(low_h, low_l, *split(u))

MESH = pl.DeviceIdType.MESH


def gather_kernel(
    order, f_ref, inv_ref, own_ref, damp_ref, ar_ref, ap_ref,
    g_ref, diag_ref, up_ref, rh, rl, load_sem, send_sem, recv_sem,
):
    s_ref = inv_ref
    row_count, z_count = lax.axis_size("row"), lax.axis_size("col") // 2
    r, c = lax.axis_index("row"), lax.axis_index("col")
    z, core = c // 2, lax.rem(c, 2)
    bpr, cols_dev = f_ref.shape[0], f_ref.shape[1]
    slab = P_SIZE // (2 * z_count)
    width = STEPS * slab
    total = s_ref.shape[0]
    per_half = total // STEPS // TILE
    left_z, right_z = lax.rem(z + z_count - 1, z_count), lax.rem(z + 1, z_count)
    far_z = lax.rem(z + 2, z_count)
    right, left, mate = (r, 2 * right_z + core), (r, 2 * left_z + core), (r, 2 * z + 1 - core)
    rx, ry, rd = [jnp.bitwise_xor(r, d) for d in (1, 2, 3)]
    x_dev, y_dev, d_dev = (rx, c), (ry, c), (rd, c)

    def load(i, b):
        return pltpu.make_async_copy(
            f_ref.at[b, pl.ds(0, width), pl.ds(0, width)], g_ref.at[b, core, z, r, pl.ds(0, width)], load_sem.at[i]
        )

    loads = [load(1, 1), load(0, 0)]
    for copy in loads:
        copy.start()
    tiles = cols_dev // TILE
    diag = [
        pltpu.make_async_copy(
            f_ref.at[core, pl.ds(t * TILE, TILE), pl.ds(t * TILE, TILE)], diag_ref.at[t], load_sem.at[2 + t]
        )
        for t in range(tiles)
    ]
    for copy in diag:
        copy.start()
    barrier = pltpu.get_barrier_semaphore()
    peers = (right, left, mate, x_dev, y_dev, d_dev)
    for peer in peers:
        pl.semaphore_signal(barrier, inc=1, device_id=peer, device_id_type=MESH)
    pl.semaphore_wait(barrier, len(peers))

    sent = []

    def send(i, ref, dev):
        copy = pltpu.make_async_remote_copy(
            src_ref=ref, dst_ref=ref, send_sem=send_sem.at[i], recv_sem=recv_sem.at[i],
            device_id=dev, device_id_type=MESH,
        )
        copy.start()
        sent.append(copy)
        return copy

    def send_to(i, src, dst, dev):
        copy = pltpu.make_async_remote_copy(
            src_ref=src, dst_ref=dst, send_sem=send_sem.at[i], recv_sem=recv_sem.at[i],
            device_id=dev, device_id_type=MESH,
        )
        copy.start()
        sent.append(copy)
        return copy

    rows = pl.ds(0, width)
    half_z = z_count // 2

    def one(z_at, r_at):
        return g_ref.at[1, core, z_at, r_at, rows]

    def plane(z_at):
        return g_ref.at[0, core, z_at]

    def plane_part(z_at, part):
        return g_ref.at[0, core, z_at, pl.ds(part * (row_count // 2), row_count // 2)]

    def column(r_at):
        return g_ref.at[1, core, :, r_at, rows]

    def column_part(r_at, part):
        return g_ref.at[1, core, pl.ds(part * half_z, half_z), r_at, rows]

    loads[0].wait()
    b_z = [send(0, one(z, r), right), send(1, one(z, r), left)]
    loads[1].wait()
    sub = lax.broadcasted_iota(jnp.int32, (8, TILE), 0)
    lane = lax.broadcasted_iota(jnp.int32, (8, TILE), 1)
    trace = jnp.zeros((8, TILE), F32)
    for t in range(tiles):
        diag[t].wait()
        for q in range(TILE // 8):
            trace = trace + jnp.where(lane == sub + 8 * q, diag_ref[t, 8 * q : 8 * q + 8, :], 0.0)
    g_ref[0, core, z, r, width:, :] = jnp.where(z == r, trace, 0.0)
    own = g_ref.at[0, core, z, r]
    a_xy = [send(2, own, x_dev), send(3, own, y_dev), send(4, own, d_dev)]

    for copy in b_z:
        copy.wait_recv()
    from_z = lax.rem(z + z_count - 1 + 2 * core, z_count)
    to_z = lax.rem(z + z_count + 1 - 2 * core, z_count)
    b_far = send(5, one(from_z, r), (r, 2 * to_z + core))
    for copy in a_xy:
        copy.wait_recv()
    a_z = [send(6, plane(z), right), send(7, plane(z), left)]
    mates = [send(8, plane(z), mate)]
    b_far.wait_recv()
    b_xy = [send(9, column(r), x_dev), send(10, column(r), y_dev)]
    mates.append(send(11, column(r), mate))
    for copy in a_z:
        copy.wait_recv()
    a_far = [send(12, plane_part(left_z, 0), right), send(13, plane_part(right_z, 1), left)]
    mates += [send(14, plane(left_z), mate), send(15, plane(right_z), mate)]
    for copy in b_xy:
        copy.wait_recv()
    b_far2 = [send(16, column_part(ry, 0), x_dev), send(17, column_part(rx, 1), y_dev)]
    mates += [send(18, column(rx), mate), send(19, column(ry), mate)]

    rest = pl.ds(width, cols_dev - width)

    def col_piece(c_at):
        return ar_ref.at[c_at, :, rest, :]

    def col_part(c_at, part):
        return ar_ref.at[c_at, part, rest, :]

    own_cols, own_rows = f_ref.at[:, rest, rows], f_ref.at[:, rows, rest]
    p_z = [send_to(20, own_cols, col_piece(c), right), send_to(21, own_cols, col_piece(c), left)]
    p_xy = [
        send_to(22, own_rows, ap_ref.at[r, :, :, rest], x_dev),
        send_to(23, own_rows, ap_ref.at[r, :, :, rest], y_dev),
    ]

    for copy in a_far:
        copy.wait_recv()
    mates += [send(24, plane_part(far_z, 0), mate), send(25, plane_part(far_z, 1), mate)]
    for copy in b_far2:
        copy.wait_recv()
    mates += [send(26, column_part(rd, 0), mate), send(27, column_part(rd, 1), mate)]
    for copy in mates:
        copy.wait_recv()
    p_mate = [send_to(28, own_cols, col_piece(c), mate)]

    low_lane = lax.broadcasted_iota(jnp.int32, (slab, TILE), 1) < slab

    def place(cb, carry):
        r_at, b = cb // bpr, lax.rem(cb, bpr)
        for z_at in range(z_count):
            for k in range(STEPS):
                one0 = g_ref[b, 0, z_at, r_at, k * slab : (k + 1) * slab, :]
                one1 = g_ref[b, 1, z_at, r_at, k * slab : (k + 1) * slab, :]
                to = pl.ds(pl.multiple_of(k * P_SIZE + cb * slab, slab), slab)
                at = z_at * 2 * slab
                if k == 0:
                    s_ref[to, at : at + 2 * slab] = jnp.where(low_lane, one0, pltpu.roll(one1, slab, 1))
                at = at + P_SIZE
                s_ref[to, at : at + 2 * slab] = jnp.where(low_lane, pltpu.roll(one0, slab, 1), one1)
        return carry

    lax.fori_loop(0, row_count * bpr, place, 0)
    trace = jnp.zeros((8, TILE), F32)
    for i in range(2):
        for j in range(z_count):
            for l in range(row_count):
                trace = trace + g_ref[0, i, j, l, width:, :]
    damping = damping_share * jnp.sum(trace) / order
    damp_ref[...] = jnp.full(damp_ref.shape, damping, F32)
    on_diag = lax.broadcasted_iota(jnp.int32, (TILE, TILE), 0) == lax.broadcasted_iota(jnp.int32, (TILE, TILE), 1)

    def damp(b, carry):
        here = at_block(b)
        s_ref[here, here] = s_ref[here, here] + jnp.where(on_diag, damping, 0.0)
        return carry

    lax.fori_loop(0, total // TILE, damp, 0)

    def factor(b, carry):
        @pl.when(b == per_half)
        def _():
            second_half(s_ref, up_ref)

        eliminate_block(b, per_half, s_ref, up_ref, rh, rl)
        return carry

    lax.fori_loop(0, total // TILE - 2, factor, 0)
    for copy in p_z + p_xy:
        copy.wait_recv()
    left_c, right_c, far_c = 2 * left_z + core, 2 * right_z + core, 2 * far_z + core
    p_far = [send(29, col_part(left_c, 0), right), send(30, col_part(right_c, 1), left)]
    p_far_xy = [send(31, ap_ref.at[ry, 0, :, rest], x_dev), send(32, ap_ref.at[rx, 1, :, rest], y_dev)]
    p_mate += [send(33, col_piece(left_c), mate), send(34, col_piece(right_c), mate)]
    lax.fori_loop(total // TILE - 2, total // TILE, factor, 0)

    columns = pl.ds(pl.multiple_of(r * bpr * slab, TILE), TILE)
    for k in range(STEPS):
        at = pl.ds(pl.multiple_of(k * P_SIZE + r * bpr * slab, TILE), TILE)
        parts = [up_ref[pl.ds(pl.multiple_of(q * P_SIZE + c * slab, slab), slab), at] for q in range(STEPS)]
        block = jnp.concatenate(parts, axis=0).T
        for b in range(bpr):
            own_ref[b, k * slab : (k + 1) * slab, :] = block[b * slab : (b + 1) * slab, :]

    for copy in p_far:
        copy.wait_recv()
    p_mate += [send(35, col_part(far_c, 0), mate), send(36, col_part(far_c, 1), mate)]
    for copy in p_far_xy + p_mate:
        copy.wait_recv()
    for copy in sent:
        copy.wait_send()


def gather_factor(factor3, order, row_count, col_count):
    bpr, cols_dev = factor3.shape[0], factor3.shape[1]
    width = STEPS * (P_SIZE // col_count)
    total = STEPS * P_SIZE
    square = jax.ShapeDtypeStruct((total, total), F32)
    vmem, hbm = pl.BlockSpec(memory_space=pltpu.VMEM), pl.BlockSpec(memory_space=pl.ANY)
    return pl.pallas_call(
        functools.partial(gather_kernel, order),
        out_shape=(
            square,
            jax.ShapeDtypeStruct((bpr, width, width), F32),
            jax.ShapeDtypeStruct((8, 128), F32),
            jax.ShapeDtypeStruct((col_count, bpr, cols_dev, width), F32),
            jax.ShapeDtypeStruct((row_count, bpr, width, cols_dev), F32),
        ),
        in_specs=[hbm],
        out_specs=(vmem, vmem, vmem, hbm, hbm),
        scratch_shapes=[
            pltpu.VMEM((bpr, 2, col_count // 2, row_count, width + 8, width), F32),
            pltpu.VMEM((cols_dev // TILE, TILE, TILE), F32),
            pltpu.VMEM((total, total), F32),
            pltpu.VMEM((TILE, total), BF16),
            pltpu.VMEM((TILE, total), BF16),
            pltpu.SemaphoreType.DMA((2 + cols_dev // TILE,)),
            pltpu.SemaphoreType.DMA((37,)),
            pltpu.SemaphoreType.DMA((37,)),
        ],
        compiler_params=pltpu.CompilerParams(
            collective_id=0, has_side_effects=True, vmem_limit_bytes=40 * 1024 * 1024
        ),
        cost_estimate=pl.CostEstimate(flops=50_000_000_000, bytes_accessed=32_000_000, transcendentals=0),
        name="gather_factor",
    )(factor3)


def in_vmem(count):
    return [pl.BlockSpec(memory_space=pltpu.VMEM)] * count


in_smem = pl.BlockSpec(memory_space=pltpu.SMEM)


def cost(flops):
    return pl.CostEstimate(flops=flops, bytes_accessed=16_000_000, transcendentals=0)


def shift(x, hops):
    count = lax.axis_size("col")
    return lax.ppermute(x, "col", [(c, (c + 2 * hops) % count) for c in range(count)])


def sibling(x):
    count = lax.axis_size("col")
    return lax.ppermute(x, "col", [(c, c ^ 1) for c in range(count)])


def ring_first(x):
    return shift(x, 1), shift(x, -1), sibling(x)


def ring_rest(x, first):
    z_count = lax.axis_size("col") // 2
    left, right, near = first
    mine, other = [x] + [None] * (z_count - 1), [near] + [None] * (z_count - 1)
    middle = z_count // 2
    from_left, from_right = x, x
    for hop in range(1, middle):
        from_left = left if hop == 1 else shift(from_left, 1)
        from_right = right if hop == 1 else shift(from_right, -1)
        mine[z_count - hop], mine[hop] = from_left, from_right
        other[z_count - hop], other[hop] = sibling(from_left), sibling(from_right)
    half = x.shape[0] // 2
    top, bottom = shift(from_left[:half], 1), shift(from_right[half:], -1)
    mine[middle] = jnp.concatenate([top, bottom], axis=0)
    other[middle] = jnp.concatenate([sibling(top), sibling(bottom)], axis=0)
    return mine, other


def across_rows(x):
    count = lax.axis_size("row")
    return [x] + [
        lax.ppermute(x, "row", [(r, r ^ d) for r in range(count)]) for d in range(1, count)
    ]


def on_device(factors):
    members = factors.shape[0]
    return jnp.stack([one_factor(factors[m]) for m in range(members)])


def one_factor(factor):
    rows_dev, cols_dev = factor.shape
    col_count, row_count = lax.axis_size("col"), lax.axis_size("row")
    z_count = col_count // 2
    order = rows_dev * row_count
    row_id, col_id = lax.axis_index("row"), lax.axis_index("col")
    z_id, core = col_id // 2, col_id % 2
    bpr = rows_dev // cols_dev
    slab = P_SIZE // col_count
    width = STEPS * slab
    total = STEPS * P_SIZE
    blocks = total // TILE
    direct = width == TILE and total == cols_dev and (row_count, z_count, bpr) == (4, 4, 2)
    if direct:
        factor3 = factor.reshape(bpr, cols_dev, cols_dev)
        inv, own, damping, ar, ap = gather_factor(factor3, order, row_count, col_count)
        return finish_update(damping, inv, own, factor3, ar, ap, slab, z_count, row_count)
    row_global = row_id * rows_dev + jnp.arange(rows_dev, dtype=jnp.int32)
    col_global = col_id * cols_dev + jnp.arange(cols_dev, dtype=jnp.int32)
    on_diagonal = row_global[:, None] == col_global[None, :]
    local_trace = jnp.sum(jnp.where(on_diagonal, factor, 0.0))

    cols = factor[:, :width]
    rows = factor.reshape(bpr, cols_dev, cols_dev)[:, :width, :]
    diag = rows[:, :, :width].reshape(bpr * width, width)
    piece = jnp.concatenate([diag, jnp.full((8, width), local_trace)], axis=0)
    slabs = jnp.stack(across_rows(piece))
    mine, other = ring_rest(slabs, ring_first(slabs))
    gathered = jnp.stack([jnp.stack(mine), jnp.stack(other)])
    gathered, cols, rows = lax.optimization_barrier((gathered, cols, rows))

    first = ring_first(cols)
    row_pieces = across_rows(rows.reshape(bpr * width, cols_dev))
    at = jnp.stack([row_id, z_id, core]).astype(jnp.int32)
    square = jax.ShapeDtypeStruct((total, total), jnp.float32)
    params = pltpu.CompilerParams(vmem_limit_bytes=40 * 1024 * 1024)
    part, low = pl.pallas_call(
        functools.partial(place_kernel, 0, blocks // 2, bpr, slab, order),
        out_shape=(square, square),
        in_specs=[in_smem] + in_vmem(1),
        out_specs=tuple(in_vmem(2)),
        compiler_params=params,
        cost_estimate=cost(30_000_000_000),
    )(at, gathered)
    part, low, first = lax.optimization_barrier((part, low, first))
    mine, other = ring_rest(cols, first)
    inv, own = pl.pallas_call(
        functools.partial(finish_kernel, blocks // 2, blocks, bpr, slab, col_count),
        out_shape=(
            jax.ShapeDtypeStruct((col_count, total, width), jnp.float32),
            jax.ShapeDtypeStruct((bpr, width, width), jnp.float32),
        ),
        in_specs=[in_smem] + in_vmem(2),
        out_specs=tuple(in_vmem(2)),
        scratch_shapes=[pltpu.VMEM((total, total), jnp.float32)] * 2,
        compiler_params=params,
        cost_estimate=cost(25_000_000_000),
    )(at, part, low)
    damping = damping_share * jnp.sum(gathered[:, :, :, bpr * width, 0]) / order

    inv_rows = [
        lax.dynamic_index_in_dim(inv, (row_id ^ d) * bpr + b, 0, keepdims=False)
        for d in range(row_count)
        for b in range(bpr)
    ]
    inv_cols = [
        lax.dynamic_index_in_dim(
            inv, (z_id + z) % z_count * 2 + (core ^ side), 0, keepdims=False
        )
        for side in range(2)
        for z in range(z_count)
    ]
    cross = dot(
        jnp.concatenate(inv_rows, axis=1), jnp.concatenate(row_pieces, axis=0), ((1,), (0,))
    )
    lower = dot(
        jnp.concatenate(mine + other, axis=1), jnp.concatenate(inv_cols, axis=1), ((1,), (1,))
    )
    update = dot(lower, cross, ((1,), (0,)), three_pass)

    lower5 = lower.reshape(rows_dev, STEPS, col_count, slab)
    new_cols = lax.dynamic_index_in_dim(lower5, col_id, 2, keepdims=False)
    new_cols = new_cols.reshape(bpr, cols_dev, width)
    new_cols = new_cols.at[:, :width, :].set(own).reshape(rows_dev, width)

    trailing = (row_global % cols_dev >= width)[:, None] & (col_global % cols_dev >= width)[None, :]
    working = factor + jnp.where(on_diagonal, damping, 0.0)
    out = jnp.where(trailing, working - update, 0.0)
    return out.at[:, :width].set(new_cols)


def solution(mesh):
    placed = (P(None, "row", "col"),)
    return jax.shard_map(
        on_device, mesh=mesh, in_specs=placed, out_specs=P(None, "row", "col"), check_vma=False
    )
```

```python
import functools

import jax
import jax.numpy as jnp
from jax import lax
from jax.experimental import pallas as pl
from jax.experimental.pallas import tpu as pltpu
from jax.sharding import PartitionSpec as P

P_SIZE = 512
STEPS = 2
TILE = 128

damping_share = 0.03162277660168379
top_precision = lax.Precision.HIGHEST
three_pass = lax.Precision.HIGH


def dot(a, b, dims, precision=top_precision):
    return lax.dot_general(
        a, b, (dims, ((), ())), precision=precision, preferred_element_type=jnp.float32
    )


def factor_tile(tile):
    size = tile.shape[0]
    groups = size // 8
    lane = lax.broadcasted_iota(jnp.int32, (8, size), 1)
    sub = lax.broadcasted_iota(jnp.int32, (8, size), 0)
    left = [tile[8 * t : 8 * t + 8, :] for t in range(groups)]
    right = [jnp.where(lane == sub + 8 * t, 1.0, 0.0).astype(jnp.float32) for t in range(groups)]

    def lanes(x, at):
        return jnp.broadcast_to(x[:, at : at + 1], x.shape)

    def rows(x, at):
        return jnp.broadcast_to(x[at : at + 1, :], x.shape)

    for j in range(groups):
        cols = [lanes(left[j], 8 * j + q) for q in range(8)]
        row_l, row_r = left[j], right[j]
        scales, coef, fin_l, fin_r = [], [], [], []
        out_l, out_r = row_l, row_r
        for i in range(8):
            pivot = rows(cols[i], i)
            s = lax.rsqrt(pivot)
            s = s * (1.5 - 0.5 * pivot * s * s)
            scales.append(s)
            l = cols[i] * s
            done_l = rows(row_l, i) * s
            done_r = rows(row_r, i) * s
            fin_l.append(done_l)
            fin_r.append(done_r)
            out_l = jnp.where(sub == i, done_l, out_l)
            out_r = jnp.where(sub == i, done_r, out_r)
            row_l = row_l - l * done_l
            row_r = row_r - l * done_r
            cq = {}
            for q in range(i + 1, 8):
                cq[q] = rows(l, q)
                cols[q] = cols[q] - l * cq[q]
            coef.append(cq)
        left[j] = jnp.where(lane >= sub + 8 * j, out_l, 0.0)
        right[j] = out_r
        for t in range(j + 1, groups):
            c = [lanes(left[t], 8 * j + q) for q in range(8)]
            acc_l, acc_r = left[t], right[t]
            for i in range(8):
                l = c[i] * scales[i]
                for q in range(i + 1, 8):
                    c[q] = c[q] - l * coef[i][q]
                acc_l = acc_l - l * fin_l[i]
                acc_r = acc_r - l * fin_r[i]
            left[t], right[t] = acc_l, acc_r
    return jnp.concatenate(left, axis=0), jnp.concatenate(right, axis=0)


def place_kernel(first_b, last_b, bpr, slab, order, at_ref, g_ref, s_ref, low_ref):
    total = STEPS * P_SIZE
    width = STEPS * slab
    per_tile = TILE // slab
    z_count, r_count = g_ref.shape[1], g_ref.shape[2]
    row_id, z_id, core = at_ref[0], at_ref[1], at_ref[2]

    def piece(r, c):
        z = lax.rem(c // 2 - z_id + z_count, z_count)
        return lax.rem(c + core, 2), z, jnp.bitwise_xor(r, row_id)

    def place(cp, carry):
        r, base = cp // bpr, (cp % bpr) * width
        for m in range(P_SIZE // TILE):
            where = [piece(r, m * per_tile + c) for c in range(per_tile)]
            for k in range(STEPS):
                got = [g_ref[i, j, l, pl.ds(base + k * slab, slab), :] for i, j, l in where]
                for kk in range(STEPS):
                    parts = [x[:, kk * slab : (kk + 1) * slab] for x in got]
                    s_ref[
                        pl.ds(pl.multiple_of(k * P_SIZE + cp * slab, 8), slab),
                        kk * P_SIZE + m * TILE : kk * P_SIZE + (m + 1) * TILE,
                    ] = jnp.concatenate(parts, axis=1)
        return carry

    lax.fori_loop(0, r_count * bpr, place, 0)
    trace = jnp.zeros((8, width), jnp.float32)
    for i in range(2):
        for j in range(z_count):
            for l in range(r_count):
                trace = trace + g_ref[i, j, l, bpr * width : bpr * width + 8, :]
    damping = damping_share * trace[0:1, 0:1] / order
    on_diag = lax.broadcasted_iota(jnp.int32, (TILE, TILE), 0) == lax.broadcasted_iota(
        jnp.int32, (TILE, TILE), 1
    )
    low_ref[...] = jnp.zeros_like(low_ref)

    def damp(b, carry):
        here = pl.ds(pl.multiple_of(b * TILE, TILE), TILE)
        tile = s_ref[here, here]
        s_ref[here, here] = tile + jnp.where(on_diag, jnp.broadcast_to(damping, tile.shape), 0.0)
        return carry

    lax.fori_loop(0, total // TILE, damp, 0)
    eliminate(first_b, last_b, s_ref, low_ref)


def eliminate(first_b, last_b, s_ref, low_ref):
    blocks = s_ref.shape[0] // TILE

    def step(b, carry):
        here = pl.ds(pl.multiple_of(b * TILE, TILE), TILE)
        upper, inverse = factor_tile(s_ref[here, here])
        low_ref[here, here] = upper.T
        s_ref[here, :] = dot(inverse, s_ref[here, :], ((1,), (0,)))
        s_ref[here, here] = inverse

        def trail(i, carry2):
            there = pl.ds(pl.multiple_of(i * TILE, TILE), TILE)
            low = dot(s_ref[there, here], inverse, ((1,), (1,)))
            low_ref[there, here] = low
            s_ref[there, here] = jnp.zeros((TILE, TILE), jnp.float32)
            s_ref[there, :] = s_ref[there, :] - dot(low, s_ref[here, :], ((1,), (0,)))
            return carry2

        lax.fori_loop(b + 1, blocks, trail, 0)
        return carry

    lax.fori_loop(first_b, last_b, step, 0)


def finish_kernel(
    first_b, last_b, bpr, slab, col_count,
    at_ref, s_in, low_in, inv_ref, own_ref, s_ref, low_ref,
):
    total = STEPS * P_SIZE
    s_ref[...] = s_in[...]
    low_ref[...] = low_in[...]
    eliminate(first_b, last_b, s_ref, low_ref)

    def emit(i, carry):
        here = pl.ds(pl.multiple_of(i * TILE, TILE), TILE)
        value = s_ref[here, :]
        col = lax.broadcasted_iota(jnp.int32, value.shape, 1)
        value = jnp.where(col < (i + 1) * TILE, value, 0.0)
        for c in range(col_count):
            parts = [value[:, k * P_SIZE + c * slab :][:, :slab] for k in range(STEPS)]
            inv_ref[c, here, :] = jnp.concatenate(parts, axis=1)
        return carry

    lax.fori_loop(0, total // TILE, emit, 0)
    row_id = at_ref[0]
    col_id = at_ref[1] * 2 + at_ref[2]
    for c in range(col_count):

        @pl.when(col_id == c)
        def _():
            for b in range(bpr):
                for k in range(STEPS):
                    at = pl.multiple_of(k * P_SIZE + (row_id * bpr + b) * slab, 8)
                    value = low_ref[pl.ds(at, slab), :]
                    parts = [value[:, q * P_SIZE + c * slab :][:, :slab] for q in range(STEPS)]
                    own_ref[b, k * slab : (k + 1) * slab, :] = jnp.concatenate(parts, axis=1)


F32, BF16 = jnp.float32, jnp.bfloat16

def split(x):
    high = x.astype(BF16)
    return high, (x - high.astype(F32)).astype(BF16)


def mul(a, b):
    return lax.dot_general(a, b, (((1,), (0,)), ((), ())), preferred_element_type=F32)


def three(a_high, a_low, b_high, b_low):
    return mul(a_high, b_high) + mul(a_low, b_high) + mul(a_high, b_low)


MB = 256


def lane_copies(x, at):
    return jnp.broadcast_to(x[:, at : at + 1], x.shape)


def row_copies(x, at):
    return jnp.broadcast_to(x[at : at + 1, :], x.shape)


def factor_small(tile):
    groups = tile.shape[0] // 8
    sub = lax.broadcasted_iota(jnp.int32, (8, tile.shape[1]), 0)
    g = [tile[8 * t : 8 * t + 8, :] for t in range(groups)]
    cols = [lane_copies(g[0], q) for q in range(8)]
    for j in range(groups):
        row = out = g[j]
        scales, coef, fin = [], [], []
        more = j + 1 < groups
        if more:
            near = [lane_copies(g[j + 1], 8 * j + q) for q in range(8)]
            after = [lane_copies(g[j + 1], 8 * j + 8 + q) for q in range(8)]
            acc = g[j + 1]
        for i in range(8):
            s = lax.rsqrt(row_copies(cols[i], i))
            l = cols[i] * s
            cq = {q: row_copies(l, q) for q in range(i + 1, 8)}
            for q in range(i + 1, 8):
                cols[q] = cols[q] - l * cq[q]
            done = row_copies(row, i) * s
            out = jnp.where(sub == i, done, out)
            row = row - l * done
            scales.append(s)
            coef.append(cq)
            fin.append(done)
            if more:
                l = near[i] * s
                for q in range(i + 1, 8):
                    near[q] = near[q] - l * cq[q]
                for q in range(8):
                    after[q] = after[q] - l * row_copies(l, q)
                acc = acc - l * done
        g[j] = out
        if more:
            g[j + 1], cols = acc, after
        for t in range(j + 2, groups):
            c = [lane_copies(g[t], 8 * j + q) for q in range(8)]
            acc = g[t]
            for i in range(8):
                l = c[i] * scales[i]
                for q in range(i + 1, 8):
                    c[q] = c[q] - l * coef[i][q]
                acc = acc - l * fin[i]
            g[t] = acc
    lane = lax.broadcasted_iota(jnp.int32, tile.shape, 1)
    height = lax.broadcasted_iota(jnp.int32, tile.shape, 0)
    return jnp.where(lane >= height, jnp.concatenate(g, axis=0), 0.0)


def dot3(a, b):
    return three(*split(a), *split(b))


def factor_block(block):
    half = TILE // 2
    eye = jnp.where(
        lax.broadcasted_iota(jnp.int32, (half, half), 0) == lax.broadcasted_iota(jnp.int32, (half, half), 1), 1.0, 0.0
    ).astype(F32)
    first = factor_small(jnp.concatenate([block[:half, :half], eye], axis=1))
    u1, i1 = first[:, :half], first[:, half:]
    cross = dot3(i1, block[:half, half:])
    low = cross.T
    second = factor_small(jnp.concatenate([block[half:, half:] - dot3(low, cross), eye], axis=1))
    u2, i2 = second[:, :half], second[:, half:]
    i21 = -dot3(i2, dot3(low, i1))
    none = jnp.zeros((half, half), F32)
    upper = jnp.concatenate(
        [jnp.concatenate([u1, cross], axis=1), jnp.concatenate([none, u2], axis=1)], axis=0
    )
    inverse = jnp.concatenate(
        [jnp.concatenate([i1, none], axis=1), jnp.concatenate([i21, i2], axis=1)], axis=0
    )
    return upper, inverse


def at_block(b):
    return pl.ds(pl.multiple_of(b * TILE, TILE), TILE)


def eliminate_block(b, per_half, s_ref, up_ref, rh, rl):
    here = at_block(b)
    upper, inverse = factor_block(s_ref[here, here])
    total = s_ref.shape[1]
    ih, il = split(inverse)
    for n in range(0, total, 256):
        cols = pl.ds(n, 256)
        value = three(ih, il, *split(s_ref[here, cols]))
        done = lax.broadcasted_iota(jnp.int32, value.shape, 1) < (b + 1) * TILE - n
        s_ref[here, cols] = jnp.where(done, value, 0.0)
        up_ref[here, cols] = jnp.where(done, 0.0, value)
        rh[:, cols], rl[:, cols] = split(value)
    up_ref[here, here] = upper
    s_ref[here, here] = inverse

    def trail(t, carry):
        there = at_block(t)
        low_h, low_l = split(up_ref[here, there].T)
        for n in range(0, total, 256):
            cols = pl.ds(n, 256)
            s_ref[there, cols] = s_ref[there, cols] - three(low_h, low_l, rh[:, cols], rl[:, cols])
        s_ref[there, here] = -three(low_h, low_l, ih, il)
        return carry

    lax.fori_loop(b + 1, (b // per_half + 1) * per_half, trail, 0)


def second_half(s_ref, up_ref):
    half = s_ref.shape[0] // 2
    for i in range(half // 256):
        rows = pl.ds(half + i * 256, 256)
        low_h, low_l = split(up_ref[0:half, rows].T)
        for n in range(half // 256):
            left, right = pl.ds(n * 256, 256), pl.ds(half + n * 256, 256)
            x = s_ref[n * 256 : half, left]
            s_ref[rows, left] = -three(low_h[:, n * 256 :], low_l[:, n * 256 :], *split(x))
            u = up_ref[0:half, right]
            s_ref[rows, right] = s_ref[rows, right] - three(low_h, low_l, *split(u))

MESH = pl.DeviceIdType.MESH


def gather_kernel(
    order, f_ref, part_ref, ar_ref, ap_ref, last_h, last_l,
    g_ref, diag_ref, s_ref, up_ref, rh, rl, a_ref, t_ref, pc_ref,
    ih, il, th, tl, xh, xl, yh, yl, wh, wl,
    load_sem, send_sem, recv_sem, pc_sem, a_sem, t_sem, o_sem, w_sem,
):
    row_count, z_count = lax.axis_size("row"), lax.axis_size("col") // 2
    r, c = lax.axis_index("row"), lax.axis_index("col")
    z, core = c // 2, lax.rem(c, 2)
    bpr, cols_dev = f_ref.shape[0], f_ref.shape[1]
    slab = P_SIZE // (2 * z_count)
    width = STEPS * slab
    total = s_ref.shape[0]
    per_half = total // STEPS // TILE
    rx, ry, rd = [jnp.bitwise_xor(r, d) for d in (1, 2, 3)]
    mate, near = (r, 2 * z + 1 - core), ((rx, c), (ry, c), (rd, c))
    reach = z_count - 1
    piece_rows = bpr * width

    loads = [
        pltpu.make_async_copy(
            f_ref.at[b, pl.ds(0, width), pl.ds(0, width)],
            g_ref.at[core, z, r, pl.ds(b * width, width)],
            load_sem.at[b],
        )
        for b in range(bpr)
    ]
    tiles = cols_dev // TILE
    loads += [
        pltpu.make_async_copy(
            f_ref.at[core, pl.ds(t * TILE, TILE), pl.ds(t * TILE, TILE)], diag_ref.at[t], load_sem.at[bpr + t]
        )
        for t in range(tiles)
    ]
    for copy in loads:
        copy.start()
    row_tiles = bpr * cols_dev // MB
    per = cols_dev // MB
    rest = pl.ds(width, cols_dev - width)

    def t_copy(t):
        return pltpu.make_async_copy(
            f_ref.at[t // per, pl.ds((t % per) * MB, MB), :], t_ref.at[pl.ds(t * MB, MB), :], t_sem.at[t]
        )

    barrier = pltpu.get_barrier_semaphore()

    def greet(dev):
        pl.semaphore_signal(barrier, inc=1, device_id=dev, device_id_type=MESH)

    for dev in (mate,) + near:
        greet(dev)
    pl.when(z > 0)(lambda: greet((r, c - 2)))
    pl.when(z < reach)(lambda: greet((r, c + 2)))
    ends_here = jnp.where(z > 0, 0, 1) + jnp.where(z < reach, 0, 1)
    pl.semaphore_wait(barrier, 3 + len(near) - ends_here)

    count = [0]

    def channel():
        count[0] += 1
        return count[0] - 1

    def remote(i, src, dst, dev):
        return pltpu.make_async_remote_copy(
            src_ref=src, dst_ref=dst, send_sem=send_sem.at[i], recv_sem=recv_sem.at[i],
            device_id=dev, device_id_type=MESH,
        )

    sent = []

    def start(i, src, dst, dev, when=None):
        copy = remote(i, src, dst, dev)
        if when is None:
            copy.start()
        else:
            pl.when(when)(copy.start)
        sent.append((when, copy))
        return copy

    def settle(copy, when=None):
        if when is None:
            copy.wait_recv()
        else:
            pl.when(when)(copy.wait_recv)

    def from_left(step):
        return z - step, z >= step, jnp.logical_and(z >= step, z < reach)

    def from_right(step):
        return z + step, z + step <= reach, jnp.logical_and(z + step <= reach, z > 0)

    def cut(z_at):
        return jnp.clip(z_at, 0, reach)

    def along(source, refs, step, part):
        ways = []
        for look, hop in ((from_left, 1), (from_right, -1)):
            z_at, here, on = look(step)
            ref = refs(cut(z_at), part)
            i = channel()
            src = source if step == 0 else ref
            start(i, src, ref, (r, c + 2 * hop), on)
            arrived_z, arrived, _ = look(step + 1)
            ref = refs(cut(arrived_z), part)
            ways.append((arrived_z, arrived, remote(i, ref, ref, mate)))
        return ways

    def pieces(z_at, part):
        return g_ref.at[core, z_at, r]

    def spread(z_at, when):
        ref = g_ref.at[core, cut(z_at), r]
        return [start(channel(), ref, ref, dev, when) for dev in near]

    def pass_on(z_at, when, copies):
        for copy in copies:
            settle(copy, when)
        ref = g_ref.at[core, cut(z_at)]
        return [(when, start(channel(), ref, ref, mate, when))]

    for copy in loads:
        copy.wait()
    sub = lax.broadcasted_iota(jnp.int32, (8, TILE), 0)
    lane = lax.broadcasted_iota(jnp.int32, (8, TILE), 1)
    trace = jnp.zeros((8, TILE), F32)
    for t in range(tiles):
        for q in range(TILE // 8):
            trace = trace + jnp.where(lane == sub + 8 * q, diag_ref[t, 8 * q : 8 * q + 8, :], 0.0)
    g_ref[core, z, r, piece_rows:, :] = jnp.where(z == r, trace, 0.0)

    mates = []
    ways = along(g_ref.at[core, z, r], pieces, 0, 0)
    waiting = [(z, None, spread(z, None))]
    own_rows = f_ref.at[:, pl.ds(0, width), rest]

    def own_cols(part):
        return f_ref.at[part, rest, pl.ds(0, width)]

    def col_part(z_at, part):
        return ar_ref.at[2 * z_at + core, part, rest, :]

    flows = [None] * bpr
    p_mate = []
    for step in range(1, z_count):
        later = []
        for z_at, here, copy in ways:
            settle(copy, here)
        if step < reach:
            onward = along(None, pieces, step, 0)
        else:
            for part in range(bpr):
                flows[part] = along(own_cols(part), col_part, 0, part)
        for z_at, here, copy in ways:
            later.append((z_at, here, spread(z_at, here)))
        for entry in waiting:
            mates += pass_on(*entry)
        waiting, ways = later, onward
    p_xy = [start(channel(), own_rows, ap_ref.at[r, :, :, rest], dev) for dev in near]
    for entry in waiting:
        mates += pass_on(*entry)
    for part in range(bpr):
        p_mate.append((None, start(channel(), own_cols(part), col_part(z, part), mate)))
    for when, copy in mates:
        settle(copy, when)

    def advance(part, step):
        for z_at, here, copy in flows[part]:
            settle(copy, here)
        old = flows[part]
        if step < reach:
            flows[part] = along(None, col_part, step, part)
        for z_at, here, copy in old:
            ref = col_part(cut(z_at), part)
            p_mate.append((here, start(channel(), ref, ref, mate, here)))

    for t in range(row_tiles):
        t_copy(t).start()

    low_lane = lax.broadcasted_iota(jnp.int32, (slab, TILE), 1) < slab

    def place(cb, carry):
        r_at, b = cb // bpr, lax.rem(cb, bpr)
        for z_at in range(z_count):
            for k in range(STEPS):
                at = pl.ds(pl.multiple_of(b * width + k * slab, slab), slab)
                one0 = g_ref[0, z_at, r_at, at, :]
                one1 = g_ref[1, z_at, r_at, at, :]
                to = pl.ds(pl.multiple_of(k * P_SIZE + cb * slab, slab), slab)
                at = z_at * 2 * slab
                if k == 0:
                    s_ref[to, at : at + 2 * slab] = jnp.where(low_lane, one0, pltpu.roll(one1, slab, 1))
                at = at + P_SIZE
                s_ref[to, at : at + 2 * slab] = jnp.where(low_lane, pltpu.roll(one0, slab, 1), one1)
        return carry

    lax.fori_loop(0, row_count * bpr, place, 0)
    trace = jnp.zeros((8, TILE), F32)
    for i in range(2):
        for j in range(z_count):
            for l in range(row_count):
                trace = trace + g_ref[i, j, l, piece_rows:, :]
    damping = damping_share * jnp.sum(trace) / order
    on_diag = lax.broadcasted_iota(jnp.int32, (TILE, TILE), 0) == lax.broadcasted_iota(jnp.int32, (TILE, TILE), 1)

    def damp(b, carry):
        here = at_block(b)
        s_ref[here, here] = s_ref[here, here] + jnp.where(on_diag, damping, 0.0)
        return carry

    lax.fori_loop(0, total // TILE, damp, 0)

    def factor(b, carry):
        @pl.when(b == per_half)
        def _():
            second_half(s_ref, up_ref)

        eliminate_block(b, per_half, s_ref, up_ref, rh, rl)
        return carry

    plan = {1: (0, 1), 3: (1, 1), 5: (0, 2), 7: (1, 2)}
    last = 0
    for b in sorted(plan):
        lax.fori_loop(last, b, factor, 0)
        advance(*plan[b])
        last = b
    lax.fori_loop(last, total // TILE, factor, 0)

    def pc_copies():
        for d in range(row_count):
            r_at = jnp.bitwise_xor(r, d)
            for b in range(bpr):
                for k in range(STEPS):
                    to = pl.multiple_of(k * P_SIZE + (r_at * bpr + b) * slab, slab)
                    at = pl.ds(k * slab, slab)
                    source = f_ref.at[b, at, rest] if d == 0 else ap_ref.at[r_at, b, at, rest]
                    yield pltpu.make_async_copy(source, pc_ref.at[pl.ds(to, slab), rest], pc_sem)

    for copy in p_xy:
        settle(copy)
    for copy in pc_copies():
        copy.start()
    pc_ref[:, 0:width] = jnp.zeros((total, width), F32)

    blocks = total // MB
    for b in range(blocks):
        for k in range(b + 1):
            here, there = pl.ds(b * MB, MB), pl.ds(k * MB, MB)
            value = s_ref[here, there]
            ih[here, there], il[here, there] = split(value)
            th[there, here], tl[there, here] = split(value.T)
    filled = pc_ref.at[:, rest]
    pltpu.make_async_copy(filled, filled, pc_sem).wait()

    def divide(i, carry):
        here = pl.ds(pl.multiple_of(i * slab, slab), slab)
        xh[here, :], xl[here, :] = split(pc_ref[here, :])
        return carry

    lax.fori_loop(0, total // slab, divide, 0)

    def forward(n, carry):
        cols = pl.ds(pl.multiple_of(n * MB, MB), MB)
        for b in range(blocks):
            here, k = pl.ds(b * MB, MB), pl.ds(0, (b + 1) * MB)
            value = three(ih[here, k], il[here, k], xh[k, cols], xl[k, cols])
            yh[here, cols], yl[here, cols] = split(value)
        return carry

    lax.fori_loop(0, cols_dev // MB, forward, 0)

    def store(sb, cols, high, low):
        k, c_at = sb // (2 * z_count), sb % (2 * z_count)
        to = arrival_slot(z, c_at // 2, reach) * 2 * width + (c_at % 2) * width + k * slab
        to = pl.ds(pl.multiple_of(to, slab), slab)
        wh[to, cols] = high
        wl[to, cols] = low

    def back(n, carry):
        cols = pl.ds(pl.multiple_of(n * MB, MB), MB)
        for b in range(blocks):
            here, k = pl.ds(b * MB, MB), pl.ds(b * MB, total - b * MB)
            high, low = split(three(th[here, k], tl[here, k], yh[k, cols], yl[k, cols]))
            for q in range(MB // slab):
                store(b * (MB // slab) + q, cols, high[q * slab : (q + 1) * slab, :], low[q * slab : (q + 1) * slab, :])
        return carry

    lax.fori_loop(0, cols_dev // MB, back, 0)
    mine = [
        s_ref[pl.ds(pl.multiple_of(k * P_SIZE + c * slab, slab), slab), :] for k in range(STEPS)
    ]
    mine = jnp.concatenate(mine, axis=0)
    for b in range(total // width):
        high, low = split(-mine[:, b * width : (b + 1) * width].T)
        for q in range(width // slab):
            store(
                b * (width // slab) + q, slice(0, width), high[q * slab : (q + 1) * slab, :], low[q * slab : (q + 1) * slab, :]
            )
    early = reach * 2 * width
    ends = [
        pltpu.make_async_copy(wh.at[pl.ds(early, 2 * width), :], last_h, w_sem.at[0]),
        pltpu.make_async_copy(wl.at[pl.ds(early, 2 * width), :], last_l, w_sem.at[1]),
    ]
    for copy in ends:
        copy.start()

    for when, copy in p_mate:
        settle(copy, when)
    settled = len(p_mate)

    def a_copies(t):
        b, first = t // per, (t % per) * MB
        skip = width if first == 0 else 0
        at = pl.ds(first + skip, MB - skip)
        for slot in range(reach):
            for side in range(2):
                to = a_ref.at[pl.ds(t * MB + skip, MB - skip), pl.ds((2 * slot + side) * width, width)]
                source = ar_ref.at[2 * arrival(z, slot, reach) + side, b, at, :]
                if slot == 0:
                    pl.when(core == side)(
                        lambda to=to: pltpu.make_async_copy(f_ref.at[b, at, pl.ds(0, width)], to, a_sem.at[t]).start()
                    )
                    pl.when(core != side)(
                        lambda to=to, source=source: pltpu.make_async_copy(source, to, a_sem.at[t]).start()
                    )
                else:
                    pltpu.make_async_copy(source, to, a_sem.at[t]).start()

    for t in range(row_tiles):
        a_copies(t)
    for b in range(bpr):
        a_ref[b * cols_dev : b * cols_dev + width, :] = jnp.zeros((width, early), F32)
    sub = lax.broadcasted_iota(jnp.int32, (MB, MB), 0)
    lane = lax.broadcasted_iota(jnp.int32, (MB, MB), 1)
    gap = lane - sub

    def out_copy(t):
        at = pl.ds(t * MB, MB)
        return pltpu.make_async_copy(t_ref.at[at, :], part_ref.at[at, :], o_sem.at[t])

    def apply(t, carry):
        here = pl.ds(pl.multiple_of(t * MB, MB), MB)
        a_high, a_low = split(a_ref[here, :])
        offset = r * bpr * cols_dev + t * MB - c * cols_dev
        for n in range(cols_dev // MB):
            cols = pl.ds(n * MB, MB)
            value = three(a_high, a_low, wh[0:early, cols], wl[0:early, cols])
            damped = t_ref[here, cols] + jnp.where(gap == offset - n * MB, damping, 0.0)
            if n == 0:
                damped = jnp.where(lane < width, 0.0, damped)
            t_ref[here, cols] = damped - value
        return carry

    own_parts = []
    for k in range(STEPS):
        at = pl.ds(pl.multiple_of(k * P_SIZE + r * bpr * slab, TILE), TILE)
        parts = [up_ref[pl.ds(pl.multiple_of(q * P_SIZE + c * slab, slab), slab), at] for q in range(STEPS)]
        own_parts.append(jnp.concatenate(parts, axis=0).T)
    for b in range(bpr):
        for i in range(per):
            t = b * per + i
            skip = width if i == 0 else 0
            filled = a_ref.at[pl.ds(t * MB + skip, MB - skip), :]
            pltpu.make_async_copy(filled, filled, a_sem.at[t]).wait()
            t_copy(t).wait()
        lax.fori_loop(b * per, (b + 1) * per, apply, 0)
        top = b * cols_dev
        for k in range(STEPS):
            t_ref[top + k * slab : top + (k + 1) * slab, 0:width] = own_parts[k][b * slab : (b + 1) * slab, :]
        t_ref[top : top + width, width:] = jnp.zeros((width, cols_dev - width), F32)
        for i in range(per):
            out_copy(b * per + i).start()
        advance(b, reach)
    for when, copy in p_mate[settled:]:
        settle(copy, when)
    for copy in ends:
        copy.wait()
    for t in range(row_tiles):
        out_copy(t).wait()
    for when, copy in sent:
        if when is None:
            copy.wait_send()
        else:
            pl.when(when)(copy.wait_send)


def arrival(z, slot, reach):
    flip = z // ((reach + 1) // 2)
    near = z + flip * (reach - 2 * z)
    base = near if slot == 0 else 1 - near if slot == 1 else slot
    return base + flip * (reach - 2 * base)


def arrival_slot(z, z_at, reach):
    flip = z // ((reach + 1) // 2)
    near = z + flip * (reach - 2 * z)
    base = z_at + flip * (reach - 2 * z_at)
    return jnp.where(base < 2, base + near * (1 - 2 * base), base)


def gather_factor(factor3, order, row_count, col_count):
    bpr, cols_dev = factor3.shape[0], factor3.shape[1]
    width = STEPS * (P_SIZE // col_count)
    total = STEPS * P_SIZE
    rows_dev = bpr * cols_dev
    late = 2 * width
    hbm = pl.BlockSpec(memory_space=pl.ANY)
    vmem_f32 = [
        (2, col_count // 2, row_count, bpr * width + 8, width),
        (cols_dev // TILE, TILE, TILE),
        (total, total),
        (total, total),
    ]
    vmem_f32_more = [(rows_dev, total - late), (rows_dev, cols_dev), (total, cols_dev)]
    tiles = rows_dev // MB
    return pl.pallas_call(
        functools.partial(gather_kernel, order),
        out_shape=(
            jax.ShapeDtypeStruct((rows_dev, cols_dev), F32),
            jax.ShapeDtypeStruct((col_count, bpr, cols_dev, width), F32),
            jax.ShapeDtypeStruct((row_count, bpr, width, cols_dev), F32),
            jax.ShapeDtypeStruct((late, cols_dev), BF16),
            jax.ShapeDtypeStruct((late, cols_dev), BF16),
        ),
        in_specs=[hbm],
        out_specs=(hbm,) * 5,
        scratch_shapes=[pltpu.VMEM(shape, F32) for shape in vmem_f32]
        + [pltpu.VMEM((TILE, total), BF16)] * 2
        + [pltpu.VMEM(shape, F32) for shape in vmem_f32_more]
        + [pltpu.VMEM((total, total), BF16)] * 4
        + [pltpu.VMEM((total, cols_dev), BF16)] * 6
        + [
            pltpu.SemaphoreType.DMA((bpr + cols_dev // TILE,)),
            pltpu.SemaphoreType.DMA((80,)),
            pltpu.SemaphoreType.DMA((80,)),
            pltpu.SemaphoreType.DMA,
            pltpu.SemaphoreType.DMA((tiles,)),
            pltpu.SemaphoreType.DMA((tiles,)),
            pltpu.SemaphoreType.DMA((tiles,)),
            pltpu.SemaphoreType.DMA((2,)),
        ],
        compiler_params=pltpu.CompilerParams(
            collective_id=0, has_side_effects=True, vmem_limit_bytes=61 * 1024 * 1024
        ),
        cost_estimate=pl.CostEstimate(flops=50_000_000_000, bytes_accessed=32_000_000, transcendentals=0),
        name="gather_factor",
    )(factor3)


def last_kernel(z_count, part_ref, ar_ref, high_ref, low_ref, out_ref, a_ref, t_ref, a_sem, t_sem, o_sem):
    c = lax.axis_index("col")
    bpr, cols_dev, width = ar_ref.shape[1:]
    reach = z_count - 1
    per = cols_dev // MB
    tiles = bpr * per
    z_last = arrival(c // 2, reach, reach)

    def rows(t):
        return pl.ds(pl.multiple_of(t * MB, MB), MB)

    def a_filled(t):
        skip = width if t % per == 0 else 0
        return pl.ds(t * MB + skip, MB - skip), skip

    def t_copy(t):
        return pltpu.make_async_copy(part_ref.at[rows(t), :], t_ref.at[rows(t), :], t_sem.at[t])

    def out_copy(t):
        return pltpu.make_async_copy(t_ref.at[rows(t), :], out_ref.at[rows(t), :], o_sem.at[t])

    for t in range(tiles):
        at, skip = a_filled(t)
        for side in range(2):
            pltpu.make_async_copy(
                ar_ref.at[2 * z_last + side, t // per, pl.ds((t % per) * MB + skip, MB - skip), :],
                a_ref.at[at, pl.ds(side * width, width)],
                a_sem.at[t],
            ).start()
        t_copy(t).start()
    for b in range(bpr):
        a_ref[b * cols_dev : b * cols_dev + width, :] = jnp.zeros((width, 2 * width), F32)

    def tile(t, carry):
        here = rows(t)
        t_copy(t).wait()
        a_high, a_low = split(a_ref[here, :])
        for n in range(cols_dev // MB):
            cols = pl.ds(n * MB, MB)
            t_ref[here, cols] = t_ref[here, cols] - three(a_high, a_low, high_ref[:, cols], low_ref[:, cols])
        out_copy(t).start()
        return carry

    for t in range(tiles):
        filled = a_ref.at[a_filled(t)[0], :]
        pltpu.make_async_copy(filled, filled, a_sem.at[t]).wait()
        if t % 2 == 1:
            lax.fori_loop(t - 1, t + 1, tile, 0)
    for t in range(tiles):
        out_copy(t).wait()


def apply_last(part, ar, high, low):
    rows_dev, cols_dev = part.shape
    tiles = rows_dev // MB
    vmem, hbm = [pl.BlockSpec(memory_space=m) for m in (pltpu.VMEM, pl.ANY)]
    return pl.pallas_call(
        functools.partial(last_kernel, ar.shape[0] // 2),
        out_shape=jax.ShapeDtypeStruct((rows_dev, cols_dev), F32),
        in_specs=[hbm, hbm, vmem, vmem],
        out_specs=hbm,
        scratch_shapes=[pltpu.VMEM((rows_dev, high.shape[0]), F32), pltpu.VMEM((rows_dev, cols_dev), F32)]
        + [pltpu.SemaphoreType.DMA((tiles,))] * 3,
        compiler_params=pltpu.CompilerParams(vmem_limit_bytes=56 * 1024 * 1024),
        cost_estimate=pl.CostEstimate(flops=3_000_000_000, bytes_accessed=20_000_000, transcendentals=0),
        name="apply_last",
    )(part, ar, high, low)


def in_vmem(count):
    return [pl.BlockSpec(memory_space=pltpu.VMEM)] * count


in_smem = pl.BlockSpec(memory_space=pltpu.SMEM)


def cost(flops):
    return pl.CostEstimate(flops=flops, bytes_accessed=16_000_000, transcendentals=0)


def shift(x, hops):
    count = lax.axis_size("col")
    return lax.ppermute(x, "col", [(c, (c + 2 * hops) % count) for c in range(count)])


def sibling(x):
    count = lax.axis_size("col")
    return lax.ppermute(x, "col", [(c, c ^ 1) for c in range(count)])


def ring_first(x):
    return shift(x, 1), shift(x, -1), sibling(x)


def ring_rest(x, first):
    z_count = lax.axis_size("col") // 2
    left, right, near = first
    mine, other = [x] + [None] * (z_count - 1), [near] + [None] * (z_count - 1)
    middle = z_count // 2
    from_left, from_right = x, x
    for hop in range(1, middle):
        from_left = left if hop == 1 else shift(from_left, 1)
        from_right = right if hop == 1 else shift(from_right, -1)
        mine[z_count - hop], mine[hop] = from_left, from_right
        other[z_count - hop], other[hop] = sibling(from_left), sibling(from_right)
    half = x.shape[0] // 2
    top, bottom = shift(from_left[:half], 1), shift(from_right[half:], -1)
    mine[middle] = jnp.concatenate([top, bottom], axis=0)
    other[middle] = jnp.concatenate([sibling(top), sibling(bottom)], axis=0)
    return mine, other


def across_rows(x):
    count = lax.axis_size("row")
    return [x] + [
        lax.ppermute(x, "row", [(r, r ^ d) for r in range(count)]) for d in range(1, count)
    ]


def on_device(factors):
    members = factors.shape[0]
    return jnp.stack([one_factor(factors[m]) for m in range(members)])


def one_factor(factor):
    rows_dev, cols_dev = factor.shape
    col_count, row_count = lax.axis_size("col"), lax.axis_size("row")
    z_count = col_count // 2
    order = rows_dev * row_count
    row_id, col_id = lax.axis_index("row"), lax.axis_index("col")
    z_id, core = col_id // 2, col_id % 2
    bpr = rows_dev // cols_dev
    slab = P_SIZE // col_count
    width = STEPS * slab
    total = STEPS * P_SIZE
    blocks = total // TILE
    direct = width == TILE and total == cols_dev and (row_count, z_count, bpr) == (4, 4, 2)
    if direct:
        factor3 = factor.reshape(bpr, cols_dev, cols_dev)
        part, ar, _, high, low = gather_factor(factor3, order, row_count, col_count)
        return apply_last(part, ar, high, low)
    row_global = row_id * rows_dev + jnp.arange(rows_dev, dtype=jnp.int32)
    col_global = col_id * cols_dev + jnp.arange(cols_dev, dtype=jnp.int32)
    on_diagonal = row_global[:, None] == col_global[None, :]
    local_trace = jnp.sum(jnp.where(on_diagonal, factor, 0.0))

    cols = factor[:, :width]
    rows = factor.reshape(bpr, cols_dev, cols_dev)[:, :width, :]
    diag = rows[:, :, :width].reshape(bpr * width, width)
    piece = jnp.concatenate([diag, jnp.full((8, width), local_trace)], axis=0)
    slabs = jnp.stack(across_rows(piece))
    mine, other = ring_rest(slabs, ring_first(slabs))
    gathered = jnp.stack([jnp.stack(mine), jnp.stack(other)])
    gathered, cols, rows = lax.optimization_barrier((gathered, cols, rows))

    first = ring_first(cols)
    row_pieces = across_rows(rows.reshape(bpr * width, cols_dev))
    at = jnp.stack([row_id, z_id, core]).astype(jnp.int32)
    square = jax.ShapeDtypeStruct((total, total), jnp.float32)
    params = pltpu.CompilerParams(vmem_limit_bytes=40 * 1024 * 1024)
    part, low = pl.pallas_call(
        functools.partial(place_kernel, 0, blocks // 2, bpr, slab, order),
        out_shape=(square, square),
        in_specs=[in_smem] + in_vmem(1),
        out_specs=tuple(in_vmem(2)),
        compiler_params=params,
        cost_estimate=cost(30_000_000_000),
    )(at, gathered)
    part, low, first = lax.optimization_barrier((part, low, first))
    mine, other = ring_rest(cols, first)
    inv, own = pl.pallas_call(
        functools.partial(finish_kernel, blocks // 2, blocks, bpr, slab, col_count),
        out_shape=(
            jax.ShapeDtypeStruct((col_count, total, width), jnp.float32),
            jax.ShapeDtypeStruct((bpr, width, width), jnp.float32),
        ),
        in_specs=[in_smem] + in_vmem(2),
        out_specs=tuple(in_vmem(2)),
        scratch_shapes=[pltpu.VMEM((total, total), jnp.float32)] * 2,
        compiler_params=params,
        cost_estimate=cost(25_000_000_000),
    )(at, part, low)
    damping = damping_share * jnp.sum(gathered[:, :, :, bpr * width, 0]) / order

    inv_rows = [
        lax.dynamic_index_in_dim(inv, (row_id ^ d) * bpr + b, 0, keepdims=False)
        for d in range(row_count)
        for b in range(bpr)
    ]
    inv_cols = [
        lax.dynamic_index_in_dim(
            inv, (z_id + z) % z_count * 2 + (core ^ side), 0, keepdims=False
        )
        for side in range(2)
        for z in range(z_count)
    ]
    cross = dot(
        jnp.concatenate(inv_rows, axis=1), jnp.concatenate(row_pieces, axis=0), ((1,), (0,))
    )
    lower = dot(
        jnp.concatenate(mine + other, axis=1), jnp.concatenate(inv_cols, axis=1), ((1,), (1,))
    )
    update = dot(lower, cross, ((1,), (0,)), three_pass)

    lower5 = lower.reshape(rows_dev, STEPS, col_count, slab)
    new_cols = lax.dynamic_index_in_dim(lower5, col_id, 2, keepdims=False)
    new_cols = new_cols.reshape(bpr, cols_dev, width)
    new_cols = new_cols.at[:, :width, :].set(own).reshape(rows_dev, width)

    trailing = (row_global % cols_dev >= width)[:, None] & (col_global % cols_dev >= width)[None, :]
    working = factor + jnp.where(on_diagonal, damping, 0.0)
    out = jnp.where(trailing, working - update, 0.0)
    return out.at[:, :width].set(new_cols)


def solution(mesh):
    placed = (P(None, "row", "col"),)
    return jax.shard_map(
        on_device, mesh=mesh, in_specs=placed, out_specs=P(None, "row", "col"), check_vma=False
    )
```

```python
import functools

import jax
import jax.numpy as jnp
from jax import lax
from jax.experimental import pallas as pl
from jax.experimental.pallas import tpu as pltpu
from jax.sharding import PartitionSpec as P

P_SIZE = 512
STEPS = 2
TILE = 128
EARLY = 3
FETCH = 7

damping_share = 0.03162277660168379
top_precision = lax.Precision.HIGHEST
three_pass = lax.Precision.HIGH


def dot(a, b, dims, precision=top_precision):
    return lax.dot_general(
        a, b, (dims, ((), ())), precision=precision, preferred_element_type=jnp.float32
    )


def factor_tile(tile):
    size = tile.shape[0]
    groups = size // 8
    lane = lax.broadcasted_iota(jnp.int32, (8, size), 1)
    sub = lax.broadcasted_iota(jnp.int32, (8, size), 0)
    left = [tile[8 * t : 8 * t + 8, :] for t in range(groups)]
    right = [jnp.where(lane == sub + 8 * t, 1.0, 0.0).astype(jnp.float32) for t in range(groups)]

    def lanes(x, at):
        return jnp.broadcast_to(x[:, at : at + 1], x.shape)

    def rows(x, at):
        return jnp.broadcast_to(x[at : at + 1, :], x.shape)

    for j in range(groups):
        cols = [lanes(left[j], 8 * j + q) for q in range(8)]
        row_l, row_r = left[j], right[j]
        scales, coef, fin_l, fin_r = [], [], [], []
        out_l, out_r = row_l, row_r
        for i in range(8):
            pivot = rows(cols[i], i)
            s = lax.rsqrt(pivot)
            s = s * (1.5 - 0.5 * pivot * s * s)
            scales.append(s)
            l = cols[i] * s
            done_l = rows(row_l, i) * s
            done_r = rows(row_r, i) * s
            fin_l.append(done_l)
            fin_r.append(done_r)
            out_l = jnp.where(sub == i, done_l, out_l)
            out_r = jnp.where(sub == i, done_r, out_r)
            row_l = row_l - l * done_l
            row_r = row_r - l * done_r
            cq = {}
            for q in range(i + 1, 8):
                cq[q] = rows(l, q)
                cols[q] = cols[q] - l * cq[q]
            coef.append(cq)
        left[j] = jnp.where(lane >= sub + 8 * j, out_l, 0.0)
        right[j] = out_r
        for t in range(j + 1, groups):
            c = [lanes(left[t], 8 * j + q) for q in range(8)]
            acc_l, acc_r = left[t], right[t]
            for i in range(8):
                l = c[i] * scales[i]
                for q in range(i + 1, 8):
                    c[q] = c[q] - l * coef[i][q]
                acc_l = acc_l - l * fin_l[i]
                acc_r = acc_r - l * fin_r[i]
            left[t], right[t] = acc_l, acc_r
    return jnp.concatenate(left, axis=0), jnp.concatenate(right, axis=0)


def place_kernel(first_b, last_b, bpr, slab, order, at_ref, g_ref, s_ref, low_ref):
    total = STEPS * P_SIZE
    width = STEPS * slab
    per_tile = TILE // slab
    z_count, r_count = g_ref.shape[1], g_ref.shape[2]
    row_id, z_id, core = at_ref[0], at_ref[1], at_ref[2]

    def piece(r, c):
        z = lax.rem(c // 2 - z_id + z_count, z_count)
        return lax.rem(c + core, 2), z, jnp.bitwise_xor(r, row_id)

    def place(cp, carry):
        r, base = cp // bpr, (cp % bpr) * width
        for m in range(P_SIZE // TILE):
            where = [piece(r, m * per_tile + c) for c in range(per_tile)]
            for k in range(STEPS):
                got = [g_ref[i, j, l, pl.ds(base + k * slab, slab), :] for i, j, l in where]
                for kk in range(STEPS):
                    parts = [x[:, kk * slab : (kk + 1) * slab] for x in got]
                    s_ref[
                        pl.ds(pl.multiple_of(k * P_SIZE + cp * slab, 8), slab),
                        kk * P_SIZE + m * TILE : kk * P_SIZE + (m + 1) * TILE,
                    ] = jnp.concatenate(parts, axis=1)
        return carry

    lax.fori_loop(0, r_count * bpr, place, 0)
    trace = jnp.zeros((8, width), jnp.float32)
    for i in range(2):
        for j in range(z_count):
            for l in range(r_count):
                trace = trace + g_ref[i, j, l, bpr * width : bpr * width + 8, :]
    damping = damping_share * trace[0:1, 0:1] / order
    on_diag = lax.broadcasted_iota(jnp.int32, (TILE, TILE), 0) == lax.broadcasted_iota(
        jnp.int32, (TILE, TILE), 1
    )
    low_ref[...] = jnp.zeros_like(low_ref)

    def damp(b, carry):
        here = pl.ds(pl.multiple_of(b * TILE, TILE), TILE)
        tile = s_ref[here, here]
        s_ref[here, here] = tile + jnp.where(on_diag, jnp.broadcast_to(damping, tile.shape), 0.0)
        return carry

    lax.fori_loop(0, total // TILE, damp, 0)
    eliminate(first_b, last_b, s_ref, low_ref)


def eliminate(first_b, last_b, s_ref, low_ref):
    blocks = s_ref.shape[0] // TILE

    def step(b, carry):
        here = pl.ds(pl.multiple_of(b * TILE, TILE), TILE)
        upper, inverse = factor_tile(s_ref[here, here])
        low_ref[here, here] = upper.T
        s_ref[here, :] = dot(inverse, s_ref[here, :], ((1,), (0,)))
        s_ref[here, here] = inverse

        def trail(i, carry2):
            there = pl.ds(pl.multiple_of(i * TILE, TILE), TILE)
            low = dot(s_ref[there, here], inverse, ((1,), (1,)))
            low_ref[there, here] = low
            s_ref[there, here] = jnp.zeros((TILE, TILE), jnp.float32)
            s_ref[there, :] = s_ref[there, :] - dot(low, s_ref[here, :], ((1,), (0,)))
            return carry2

        lax.fori_loop(b + 1, blocks, trail, 0)
        return carry

    lax.fori_loop(first_b, last_b, step, 0)


def finish_kernel(
    first_b, last_b, bpr, slab, col_count,
    at_ref, s_in, low_in, inv_ref, own_ref, s_ref, low_ref,
):
    total = STEPS * P_SIZE
    s_ref[...] = s_in[...]
    low_ref[...] = low_in[...]
    eliminate(first_b, last_b, s_ref, low_ref)

    def emit(i, carry):
        here = pl.ds(pl.multiple_of(i * TILE, TILE), TILE)
        value = s_ref[here, :]
        col = lax.broadcasted_iota(jnp.int32, value.shape, 1)
        value = jnp.where(col < (i + 1) * TILE, value, 0.0)
        for c in range(col_count):
            parts = [value[:, k * P_SIZE + c * slab :][:, :slab] for k in range(STEPS)]
            inv_ref[c, here, :] = jnp.concatenate(parts, axis=1)
        return carry

    lax.fori_loop(0, total // TILE, emit, 0)
    row_id = at_ref[0]
    col_id = at_ref[1] * 2 + at_ref[2]
    for c in range(col_count):

        @pl.when(col_id == c)
        def _():
            for b in range(bpr):
                for k in range(STEPS):
                    at = pl.multiple_of(k * P_SIZE + (row_id * bpr + b) * slab, 8)
                    value = low_ref[pl.ds(at, slab), :]
                    parts = [value[:, q * P_SIZE + c * slab :][:, :slab] for q in range(STEPS)]
                    own_ref[b, k * slab : (k + 1) * slab, :] = jnp.concatenate(parts, axis=1)


F32, BF16 = jnp.float32, jnp.bfloat16

def split(x):
    high = x.astype(BF16)
    return high, (x - high.astype(F32)).astype(BF16)


def mul(a, b):
    return lax.dot_general(a, b, (((1,), (0,)), ((), ())), preferred_element_type=F32)


def three(a_high, a_low, b_high, b_low):
    return mul(a_high, b_high) + mul(a_low, b_high) + mul(a_high, b_low)


MB = 256


def lane_copies(x, at):
    return jnp.broadcast_to(x[:, at : at + 1], x.shape)


def row_copies(x, at):
    return jnp.broadcast_to(x[at : at + 1, :], x.shape)


def factor_small(tile):
    groups = tile.shape[0] // 8
    sub = lax.broadcasted_iota(jnp.int32, (8, tile.shape[1]), 0)
    g = [tile[8 * t : 8 * t + 8, :] for t in range(groups)]
    cols = [lane_copies(g[0], q) for q in range(8)]
    for j in range(groups):
        row = out = g[j]
        scales, coef, fin = [], [], []
        more = j + 1 < groups
        if more:
            near = [lane_copies(g[j + 1], 8 * j + q) for q in range(8)]
            after = [lane_copies(g[j + 1], 8 * j + 8 + q) for q in range(8)]
            acc = g[j + 1]
        for i in range(8):
            s = lax.rsqrt(row_copies(cols[i], i))
            l = cols[i] * s
            cq = {q: row_copies(l, q) for q in range(i + 1, 8)}
            for q in range(i + 1, 8):
                cols[q] = cols[q] - l * cq[q]
            done = row_copies(row, i) * s
            out = jnp.where(sub == i, done, out)
            row = row - l * done
            scales.append(s)
            coef.append(cq)
            fin.append(done)
            if more:
                l = near[i] * s
                for q in range(i + 1, 8):
                    near[q] = near[q] - l * cq[q]
                for q in range(8):
                    after[q] = after[q] - l * row_copies(l, q)
                acc = acc - l * done
        g[j] = out
        if more:
            g[j + 1], cols = acc, after
        for t in range(j + 2, groups):
            c = [lane_copies(g[t], 8 * j + q) for q in range(8)]
            acc = g[t]
            for i in range(8):
                l = c[i] * scales[i]
                for q in range(i + 1, 8):
                    c[q] = c[q] - l * coef[i][q]
                acc = acc - l * fin[i]
            g[t] = acc
    lane = lax.broadcasted_iota(jnp.int32, tile.shape, 1)
    height = lax.broadcasted_iota(jnp.int32, tile.shape, 0)
    return jnp.where(lane >= height, jnp.concatenate(g, axis=0), 0.0)


def dot3(a, b):
    return three(*split(a), *split(b))


def factor_block(block):
    half = TILE // 2
    eye = jnp.where(
        lax.broadcasted_iota(jnp.int32, (half, half), 0) == lax.broadcasted_iota(jnp.int32, (half, half), 1), 1.0, 0.0
    ).astype(F32)
    first = factor_small(jnp.concatenate([block[:half, :half], eye], axis=1))
    u1, i1 = first[:, :half], first[:, half:]
    cross = dot3(i1, block[:half, half:])
    low = cross.T
    second = factor_small(jnp.concatenate([block[half:, half:] - dot3(low, cross), eye], axis=1))
    u2, i2 = second[:, :half], second[:, half:]
    i21 = -dot3(i2, dot3(low, i1))
    none = jnp.zeros((half, half), F32)
    upper = jnp.concatenate(
        [jnp.concatenate([u1, cross], axis=1), jnp.concatenate([none, u2], axis=1)], axis=0
    )
    inverse = jnp.concatenate(
        [jnp.concatenate([i1, none], axis=1), jnp.concatenate([i21, i2], axis=1)], axis=0
    )
    return upper, inverse


def at_block(b):
    return pl.ds(pl.multiple_of(b * TILE, TILE), TILE)


def eliminate_block(b, per_half, s_ref, up_ref, rh, rl):
    here = at_block(b)
    upper, inverse = factor_block(s_ref[here, here])
    total = s_ref.shape[1]
    ih, il = split(inverse)
    for n in range(0, total, 256):
        cols = pl.ds(n, 256)
        value = three(ih, il, *split(s_ref[here, cols]))
        done = lax.broadcasted_iota(jnp.int32, value.shape, 1) < (b + 1) * TILE - n
        s_ref[here, cols] = jnp.where(done, value, 0.0)
        up_ref[here, cols] = jnp.where(done, 0.0, value)
        rh[:, cols], rl[:, cols] = split(value)
    up_ref[here, here] = upper
    s_ref[here, here] = inverse

    def trail(t, carry):
        there = at_block(t)
        low_h, low_l = split(up_ref[here, there].T)
        for n in range(0, total, 256):
            cols = pl.ds(n, 256)
            s_ref[there, cols] = s_ref[there, cols] - three(low_h, low_l, rh[:, cols], rl[:, cols])
        s_ref[there, here] = -three(low_h, low_l, ih, il)
        return carry

    lax.fori_loop(b + 1, (b // per_half + 1) * per_half, trail, 0)


def second_half(s_ref, up_ref):
    half = s_ref.shape[0] // 2
    for i in range(half // 256):
        rows = pl.ds(half + i * 256, 256)
        low_h, low_l = split(up_ref[0:half, rows].T)
        for n in range(half // 256):
            left, right = pl.ds(n * 256, 256), pl.ds(half + n * 256, 256)
            x = s_ref[n * 256 : half, left]
            s_ref[rows, left] = -three(low_h[:, n * 256 :], low_l[:, n * 256 :], *split(x))
            u = up_ref[0:half, right]
            s_ref[rows, right] = s_ref[rows, right] - three(low_h, low_l, *split(u))

MESH = pl.DeviceIdType.MESH


def gather_kernel(
    order, f_ref, part_ref, ar_ref, ap_ref, last_h, last_l,
    g_ref, diag_ref, s_ref, up_ref, rh, rl, a_ref, t_ref, pc_ref,
    ih, il, th, tl, xh, xl, yh, yl, wh, wl,
    load_sem, send_sem, recv_sem, pc_sem, a_sem, t_sem, o_sem, w_sem,
):
    row_count, z_count = lax.axis_size("row"), lax.axis_size("col") // 2
    r, c = lax.axis_index("row"), lax.axis_index("col")
    z, core = c // 2, lax.rem(c, 2)
    bpr, cols_dev = f_ref.shape[0], f_ref.shape[1]
    slab = P_SIZE // (2 * z_count)
    width = STEPS * slab
    total = s_ref.shape[0]
    per_half = total // STEPS // TILE
    rx, ry = jnp.bitwise_xor(r, 1), jnp.bitwise_xor(r, 2)
    x_dev, y_dev, mate = (rx, c), (ry, c), (r, 2 * z + 1 - core)
    near = (x_dev, y_dev)
    reach = z_count - 1
    piece_rows = bpr * width
    upper_rows = piece_rows // 2

    loads = [
        pltpu.make_async_copy(
            f_ref.at[b, pl.ds(0, width), pl.ds(0, width)],
            g_ref.at[core, z, r, pl.ds(b * width, width)],
            load_sem.at[b],
        )
        for b in range(bpr)
    ]
    tiles = cols_dev // TILE
    loads += [
        pltpu.make_async_copy(
            f_ref.at[core, pl.ds(t * TILE, TILE), pl.ds(t * TILE, TILE)], diag_ref.at[t], load_sem.at[bpr + t]
        )
        for t in range(tiles)
    ]
    for copy in loads:
        copy.start()
    row_tiles = bpr * cols_dev // MB
    per = cols_dev // MB
    rest = pl.ds(width, cols_dev - width)

    def t_copy(t):
        return pltpu.make_async_copy(
            f_ref.at[t // per, pl.ds((t % per) * MB, MB), :], t_ref.at[pl.ds(t * MB, MB), :], t_sem.at[t]
        )

    barrier = pltpu.get_barrier_semaphore()

    def greet(dev):
        pl.semaphore_signal(barrier, inc=1, device_id=dev, device_id_type=MESH)

    for dev in (mate,) + near:
        greet(dev)
    pl.when(z > 0)(lambda: greet((r, c - 2)))
    pl.when(z < reach)(lambda: greet((r, c + 2)))
    ends_here = jnp.where(z > 0, 0, 1) + jnp.where(z < reach, 0, 1)
    pl.semaphore_wait(barrier, 3 + len(near) - ends_here)

    count = [0]

    def channel():
        count[0] += 1
        return count[0] - 1

    def remote(i, src, dst, dev):
        return pltpu.make_async_remote_copy(
            src_ref=src, dst_ref=dst, send_sem=send_sem.at[i], recv_sem=recv_sem.at[i],
            device_id=dev, device_id_type=MESH,
        )

    sent = []

    def start(i, src, dst, dev, when=None):
        copy = remote(i, src, dst, dev)
        if when is None:
            copy.start()
        else:
            pl.when(when)(copy.start)
        sent.append((when, copy))
        return copy

    def settle(copy, when=None):
        if when is None:
            copy.wait_recv()
        else:
            pl.when(when)(copy.wait_recv)

    def from_left(step):
        return z - step, z >= step, jnp.logical_and(z >= step, z < reach)

    def from_right(step):
        return z + step, z + step <= reach, jnp.logical_and(z + step <= reach, z > 0)

    def cut(z_at):
        return jnp.clip(z_at, 0, reach)

    def along(source, refs, step, part):
        ways = []
        for look, hop in ((from_left, 1), (from_right, -1)):
            z_at, here, on = look(step)
            ref = refs(cut(z_at), part)
            i = channel()
            src = source if step == 0 else ref
            start(i, src, ref, (r, c + 2 * hop), on)
            arrived_z, arrived, _ = look(step + 1)
            ref = refs(cut(arrived_z), part)
            ways.append((arrived_z, arrived, remote(i, ref, ref, mate)))
        return ways

    def pieces(z_at, part):
        return g_ref.at[core, z_at, r]

    def spread(z_at, when):
        ref = g_ref.at[core, cut(z_at), r]
        return [start(channel(), ref, ref, dev, when) for dev in (x_dev, y_dev)]

    def relay(z_at, when, copies):
        for copy in copies:
            settle(copy, when)
        top = g_ref.at[core, cut(z_at), ry, pl.ds(0, upper_rows)]
        bottom = g_ref.at[core, cut(z_at), rx, pl.ds(upper_rows, piece_rows + 8 - upper_rows)]
        return [start(channel(), top, top, x_dev, when), start(channel(), bottom, bottom, y_dev, when)]

    def pass_on(z_at, when, copies):
        for copy in copies:
            settle(copy, when)
        ref = g_ref.at[core, cut(z_at)]
        return [(when, start(channel(), ref, ref, mate, when))]

    for copy in loads:
        copy.wait()
    sub = lax.broadcasted_iota(jnp.int32, (8, TILE), 0)
    lane = lax.broadcasted_iota(jnp.int32, (8, TILE), 1)
    trace = jnp.zeros((8, TILE), F32)
    for t in range(tiles):
        for q in range(TILE // 8):
            trace = trace + jnp.where(lane == sub + 8 * q, diag_ref[t, 8 * q : 8 * q + 8, :], 0.0)
    g_ref[core, z, r, piece_rows:, :] = jnp.where(z == r, trace, 0.0)

    mates = []
    ways = along(g_ref.at[core, z, r], pieces, 0, 0)
    waiting, relayed = [(z, None, spread(z, None))], []
    own_rows = f_ref.at[:, pl.ds(0, width), rest]

    def own_cols(part):
        return f_ref.at[part, rest, pl.ds(0, width)]

    def col_part(z_at, part):
        return ar_ref.at[2 * z_at + core, part, rest, :]

    flows = [None] * bpr
    p_mate = []
    for step in range(1, z_count):
        later = []
        for z_at, here, copy in ways:
            settle(copy, here)
        if step < reach:
            onward = along(None, pieces, step, 0)
        else:
            for part in range(bpr):
                flows[part] = along(own_cols(part), col_part, 0, part)
        for z_at, here, copy in ways:
            later.append((z_at, here, spread(z_at, here)))
        for entry in relayed:
            mates += pass_on(*entry)
        relayed = [(z_at, when, relay(z_at, when, copies)) for z_at, when, copies in waiting]
        waiting, ways = later, onward
    relayed += [(z_at, when, relay(z_at, when, copies)) for z_at, when, copies in waiting]
    p_xy = [start(channel(), own_rows, ap_ref.at[r, :, :, rest], dev) for dev in near]
    for entry in relayed:
        mates += pass_on(*entry)
    for part in range(bpr):
        p_mate.append((None, start(channel(), own_cols(part), col_part(z, part), mate)))
    for when, copy in mates:
        settle(copy, when)

    def advance(part, step):
        for z_at, here, copy in flows[part]:
            settle(copy, here)
        old = flows[part]
        if step < reach:
            flows[part] = along(None, col_part, step, part)
        for z_at, here, copy in old:
            ref = col_part(cut(z_at), part)
            p_mate.append((here, start(channel(), ref, ref, mate, here)))

    for t in range(row_tiles):
        t_copy(t).start()

    low_lane = lax.broadcasted_iota(jnp.int32, (slab, TILE), 1) < slab

    def place(cb, carry):
        r_at, b = cb // bpr, lax.rem(cb, bpr)
        for z_at in range(z_count):
            for k in range(STEPS):
                at = pl.ds(pl.multiple_of(b * width + k * slab, slab), slab)
                one0 = g_ref[0, z_at, r_at, at, :]
                one1 = g_ref[1, z_at, r_at, at, :]
                to = pl.ds(pl.multiple_of(k * P_SIZE + cb * slab, slab), slab)
                at = z_at * 2 * slab
                if k == 0:
                    s_ref[to, at : at + 2 * slab] = jnp.where(low_lane, one0, pltpu.roll(one1, slab, 1))
                at = at + P_SIZE
                s_ref[to, at : at + 2 * slab] = jnp.where(low_lane, pltpu.roll(one0, slab, 1), one1)
        return carry

    lax.fori_loop(0, row_count * bpr, place, 0)
    trace = jnp.zeros((8, TILE), F32)
    for i in range(2):
        for j in range(z_count):
            for l in range(row_count):
                trace = trace + g_ref[i, j, l, piece_rows:, :]
    damping = damping_share * jnp.sum(trace) / order
    on_diag = lax.broadcasted_iota(jnp.int32, (TILE, TILE), 0) == lax.broadcasted_iota(jnp.int32, (TILE, TILE), 1)

    def damp(b, carry):
        here = at_block(b)
        s_ref[here, here] = s_ref[here, here] + jnp.where(on_diag, damping, 0.0)
        return carry

    lax.fori_loop(0, total // TILE, damp, 0)

    def factor(b, carry):
        @pl.when(b == per_half)
        def _():
            second_half(s_ref, up_ref)

        eliminate_block(b, per_half, s_ref, up_ref, rh, rl)
        return carry

    early = EARLY * 2 * width

    def a_copies(t, slots):
        b, first = t // per, (t % per) * MB
        skip = width if first == 0 else 0
        at = pl.ds(first + skip, MB - skip)
        for slot in slots:
            for side in range(2):
                to = a_ref.at[pl.ds(t * MB + skip, MB - skip), pl.ds((2 * slot + side) * width, width)]
                source = ar_ref.at[2 * arrival(z, slot, reach) + side, b, at, :]
                if slot == 0:
                    pl.when(core == side)(
                        lambda to=to: pltpu.make_async_copy(f_ref.at[b, at, pl.ds(0, width)], to, a_sem.at[t]).start()
                    )
                    pl.when(core != side)(
                        lambda to=to, source=source: pltpu.make_async_copy(source, to, a_sem.at[t]).start()
                    )
                else:
                    pltpu.make_async_copy(source, to, a_sem.at[t]).start()

    def pc_copies():
        for d in range(row_count):
            r_at = jnp.bitwise_xor(r, d)
            for b in range(bpr):
                for k in range(STEPS):
                    to = pl.multiple_of(k * P_SIZE + (r_at * bpr + b) * slab, slab)
                    at = pl.ds(k * slab, slab)
                    source = f_ref.at[b, at, rest] if d == 0 else ap_ref.at[r_at, b, at, rest]
                    yield pltpu.make_async_copy(source, pc_ref.at[pl.ds(to, slab), rest], pc_sem)

    def fetch_first():
        for when, copy in p_mate:
            settle(copy, when)
        for t in range(row_tiles):
            a_copies(t, range(2))
        for copy in p_xy:
            settle(copy)
        for copy in pc_copies():
            copy.start()
        for b in range(bpr):
            a_ref[b * cols_dev : b * cols_dev + width, :] = jnp.zeros((width, early), F32)
        pc_ref[:, 0:width] = jnp.zeros((total, width), F32)
        return len(p_mate)

    plan = {1: (0, 1), 3: (1, 1), 5: (0, 2), 7: (1, 2)}
    last = 0
    for b in sorted(plan):
        lax.fori_loop(last, b, factor, 0)
        if b == 3:
            for copy in p_xy:
                settle(copy)
            top, bottom = ap_ref.at[ry, 0, :, rest], ap_ref.at[rx, 1, :, rest]
            p_xy = [start(channel(), top, top, x_dev), start(channel(), bottom, bottom, y_dev)]
        if b == FETCH:
            settled = fetch_first()
        advance(*plan[b])
        last = b
    lax.fori_loop(last, total // TILE, factor, 0)
    filled = pc_ref.at[:, rest]
    pltpu.make_async_copy(filled, filled, pc_sem).wait()

    def divide(i, carry):
        here = pl.ds(pl.multiple_of(i * slab, slab), slab)
        xh[here, :], xl[here, :] = split(pc_ref[here, :])
        return carry

    lax.fori_loop(0, total // slab, divide, 0)

    blocks = total // MB
    for b in range(blocks):
        for k in range(b + 1):
            here, there = pl.ds(b * MB, MB), pl.ds(k * MB, MB)
            value = s_ref[here, there]
            ih[here, there], il[here, there] = split(value)
            th[there, here], tl[there, here] = split(value.T)
    def forward(n, carry):
        cols = pl.ds(pl.multiple_of(n * MB, MB), MB)
        for b in range(blocks):
            here, k = pl.ds(b * MB, MB), pl.ds(0, (b + 1) * MB)
            value = three(ih[here, k], il[here, k], xh[k, cols], xl[k, cols])
            yh[here, cols], yl[here, cols] = split(value)
        return carry

    lax.fori_loop(0, cols_dev // MB, forward, 0)
    if EARLY > 2:
        for when, copy in p_mate[settled:]:
            settle(copy, when)
        settled = len(p_mate)
        for t in range(row_tiles):
            a_copies(t, range(2, EARLY))

    def store(sb, cols, high, low):
        k, c_at = sb // (2 * z_count), sb % (2 * z_count)
        to = arrival_slot(z, c_at // 2, reach) * 2 * width + (c_at % 2) * width + k * slab
        to = pl.ds(pl.multiple_of(to, slab), slab)
        wh[to, cols] = high
        wl[to, cols] = low

    def back(n, carry):
        cols = pl.ds(pl.multiple_of(n * MB, MB), MB)
        for b in range(blocks):
            here, k = pl.ds(b * MB, MB), pl.ds(b * MB, total - b * MB)
            high, low = split(three(th[here, k], tl[here, k], yh[k, cols], yl[k, cols]))
            for q in range(MB // slab):
                store(b * (MB // slab) + q, cols, high[q * slab : (q + 1) * slab, :], low[q * slab : (q + 1) * slab, :])
        return carry

    lax.fori_loop(0, cols_dev // MB, back, 0)
    mine = [
        s_ref[pl.ds(pl.multiple_of(k * P_SIZE + c * slab, slab), slab), :] for k in range(STEPS)
    ]
    mine = jnp.concatenate(mine, axis=0)
    for b in range(total // width):
        high, low = split(-mine[:, b * width : (b + 1) * width].T)
        for q in range(width // slab):
            store(
                b * (width // slab) + q, slice(0, width), high[q * slab : (q + 1) * slab, :], low[q * slab : (q + 1) * slab, :]
            )
    ends = [
        pltpu.make_async_copy(wh.at[pl.ds(early, total - early), :], last_h, w_sem.at[0]),
        pltpu.make_async_copy(wl.at[pl.ds(early, total - early), :], last_l, w_sem.at[1]),
    ]
    for copy in ends:
        copy.start()

    sub = lax.broadcasted_iota(jnp.int32, (MB, MB), 0)
    lane = lax.broadcasted_iota(jnp.int32, (MB, MB), 1)
    gap = lane - sub

    def out_copy(t):
        at = pl.ds(t * MB, MB)
        return pltpu.make_async_copy(t_ref.at[at, :], part_ref.at[at, :], o_sem.at[t])

    def apply(t, carry):
        here = pl.ds(pl.multiple_of(t * MB, MB), MB)
        a_high, a_low = split(a_ref[here, :])
        offset = r * bpr * cols_dev + t * MB - c * cols_dev
        for n in range(cols_dev // MB):
            cols = pl.ds(n * MB, MB)
            value = three(a_high, a_low, wh[0:early, cols], wl[0:early, cols])
            damped = t_ref[here, cols] + jnp.where(gap == offset - n * MB, damping, 0.0)
            if n == 0:
                damped = jnp.where(lane < width, 0.0, damped)
            t_ref[here, cols] = damped - value
        return carry

    own_parts = []
    for k in range(STEPS):
        at = pl.ds(pl.multiple_of(k * P_SIZE + r * bpr * slab, TILE), TILE)
        parts = [up_ref[pl.ds(pl.multiple_of(q * P_SIZE + c * slab, slab), slab), at] for q in range(STEPS)]
        own_parts.append(jnp.concatenate(parts, axis=0).T)
    for b in range(bpr):
        for i in range(per):
            t = b * per + i
            skip = width if i == 0 else 0
            filled = a_ref.at[pl.ds(t * MB + skip, MB - skip), :]
            pltpu.make_async_copy(filled, filled, a_sem.at[t]).wait()
            t_copy(t).wait()
        advance(b, reach)
        lax.fori_loop(b * per, (b + 1) * per, apply, 0)
        top = b * cols_dev
        for k in range(STEPS):
            t_ref[top + k * slab : top + (k + 1) * slab, 0:width] = own_parts[k][b * slab : (b + 1) * slab, :]
        t_ref[top : top + width, width:] = jnp.zeros((width, cols_dev - width), F32)
        for i in range(per):
            out_copy(b * per + i).start()
    for when, copy in p_mate[settled:]:
        settle(copy, when)
    for copy in ends:
        copy.wait()
    for t in range(row_tiles):
        out_copy(t).wait()
    for when, copy in sent:
        if when is None:
            copy.wait_send()
        else:
            pl.when(when)(copy.wait_send)


def arrival(z, slot, reach):
    flip = z // ((reach + 1) // 2)
    near = z + flip * (reach - 2 * z)
    base = near if slot == 0 else 1 - near if slot == 1 else slot
    return base + flip * (reach - 2 * base)


def arrival_slot(z, z_at, reach):
    flip = z // ((reach + 1) // 2)
    near = z + flip * (reach - 2 * z)
    base = z_at + flip * (reach - 2 * z_at)
    return jnp.where(base < 2, base + near * (1 - 2 * base), base)


def gather_factor(factor3, order, row_count, col_count):
    bpr, cols_dev = factor3.shape[0], factor3.shape[1]
    width = STEPS * (P_SIZE // col_count)
    total = STEPS * P_SIZE
    rows_dev = bpr * cols_dev
    late = total - EARLY * 2 * width
    hbm = pl.BlockSpec(memory_space=pl.ANY)
    vmem_f32 = [
        (2, col_count // 2, row_count, bpr * width + 8, width),
        (cols_dev // TILE, TILE, TILE),
        (total, total),
        (total, total),
    ]
    vmem_f32_more = [(rows_dev, total - late), (rows_dev, cols_dev), (total, cols_dev)]
    tiles = rows_dev // MB
    return pl.pallas_call(
        functools.partial(gather_kernel, order),
        out_shape=(
            jax.ShapeDtypeStruct((rows_dev, cols_dev), F32),
            jax.ShapeDtypeStruct((col_count, bpr, cols_dev, width), F32),
            jax.ShapeDtypeStruct((row_count, bpr, width, cols_dev), F32),
            jax.ShapeDtypeStruct((late, cols_dev), BF16),
            jax.ShapeDtypeStruct((late, cols_dev), BF16),
        ),
        in_specs=[hbm],
        out_specs=(hbm,) * 5,
        scratch_shapes=[pltpu.VMEM(shape, F32) for shape in vmem_f32]
        + [pltpu.VMEM((TILE, total), BF16)] * 2
        + [pltpu.VMEM(shape, F32) for shape in vmem_f32_more]
        + [pltpu.VMEM((total, total), BF16)] * 4
        + [pltpu.VMEM((total, cols_dev), BF16)] * 6
        + [
            pltpu.SemaphoreType.DMA((bpr + cols_dev // TILE,)),
            pltpu.SemaphoreType.DMA((80,)),
            pltpu.SemaphoreType.DMA((80,)),
            pltpu.SemaphoreType.DMA,
            pltpu.SemaphoreType.DMA((tiles,)),
            pltpu.SemaphoreType.DMA((tiles,)),
            pltpu.SemaphoreType.DMA((tiles,)),
            pltpu.SemaphoreType.DMA((2,)),
        ],
        compiler_params=pltpu.CompilerParams(
            collective_id=0, has_side_effects=True, vmem_limit_bytes=61 * 1024 * 1024
        ),
        cost_estimate=pl.CostEstimate(flops=50_000_000_000, bytes_accessed=32_000_000, transcendentals=0),
        name="gather_factor",
    )(factor3)


def last_kernel(z_count, part_ref, ar_ref, high_ref, low_ref, out_ref, a_ref, t_ref, a_sem, t_sem, o_sem):
    c = lax.axis_index("col")
    bpr, cols_dev, width = ar_ref.shape[1:]
    reach = z_count - 1
    per = cols_dev // MB
    tiles = bpr * per

    def rows(t):
        return pl.ds(pl.multiple_of(t * MB, MB), MB)

    def a_filled(t):
        skip = width if t % per == 0 else 0
        return pl.ds(t * MB + skip, MB - skip), skip

    def t_copy(t):
        return pltpu.make_async_copy(part_ref.at[rows(t), :], t_ref.at[rows(t), :], t_sem.at[t])

    def out_copy(t):
        return pltpu.make_async_copy(t_ref.at[rows(t), :], out_ref.at[rows(t), :], o_sem.at[t])

    for t in range(tiles):
        at, skip = a_filled(t)
        for j in range(2 * (z_count - EARLY)):
            c_at = 2 * arrival(c // 2, EARLY + j // 2, reach) + j % 2
            pltpu.make_async_copy(
                ar_ref.at[c_at, t // per, pl.ds((t % per) * MB + skip, MB - skip), :],
                a_ref.at[at, pl.ds(j * width, width)],
                a_sem.at[t],
            ).start()
        t_copy(t).start()
    for b in range(bpr):
        a_ref[b * cols_dev : b * cols_dev + width, :] = jnp.zeros((width, a_ref.shape[1]), F32)

    def tile(t, carry):
        here = rows(t)
        t_copy(t).wait()
        a_high, a_low = split(a_ref[here, :])
        for n in range(cols_dev // MB):
            cols = pl.ds(n * MB, MB)
            t_ref[here, cols] = t_ref[here, cols] - three(a_high, a_low, high_ref[:, cols], low_ref[:, cols])
        out_copy(t).start()
        return carry

    for t in range(tiles):
        filled = a_ref.at[a_filled(t)[0], :]
        pltpu.make_async_copy(filled, filled, a_sem.at[t]).wait()
        if t % 2 == 1:
            lax.fori_loop(t - 1, t + 1, tile, 0)
    for t in range(tiles):
        out_copy(t).wait()


def apply_last(part, ar, high, low):
    rows_dev, cols_dev = part.shape
    tiles = rows_dev // MB
    vmem, hbm = [pl.BlockSpec(memory_space=m) for m in (pltpu.VMEM, pl.ANY)]
    return pl.pallas_call(
        functools.partial(last_kernel, ar.shape[0] // 2),
        out_shape=jax.ShapeDtypeStruct((rows_dev, cols_dev), F32),
        in_specs=[hbm, hbm, vmem, vmem],
        out_specs=hbm,
        scratch_shapes=[pltpu.VMEM((rows_dev, high.shape[0]), F32), pltpu.VMEM((rows_dev, cols_dev), F32)]
        + [pltpu.SemaphoreType.DMA((tiles,))] * 3,
        compiler_params=pltpu.CompilerParams(vmem_limit_bytes=56 * 1024 * 1024),
        cost_estimate=pl.CostEstimate(flops=6_000_000_000, bytes_accessed=20_000_000, transcendentals=0),
        name="apply_last",
    )(part, ar, high, low)


def in_vmem(count):
    return [pl.BlockSpec(memory_space=pltpu.VMEM)] * count


in_smem = pl.BlockSpec(memory_space=pltpu.SMEM)


def cost(flops):
    return pl.CostEstimate(flops=flops, bytes_accessed=16_000_000, transcendentals=0)


def shift(x, hops):
    count = lax.axis_size("col")
    return lax.ppermute(x, "col", [(c, (c + 2 * hops) % count) for c in range(count)])


def sibling(x):
    count = lax.axis_size("col")
    return lax.ppermute(x, "col", [(c, c ^ 1) for c in range(count)])


def ring_first(x):
    return shift(x, 1), shift(x, -1), sibling(x)


def ring_rest(x, first):
    z_count = lax.axis_size("col") // 2
    left, right, near = first
    mine, other = [x] + [None] * (z_count - 1), [near] + [None] * (z_count - 1)
    middle = z_count // 2
    from_left, from_right = x, x
    for hop in range(1, middle):
        from_left = left if hop == 1 else shift(from_left, 1)
        from_right = right if hop == 1 else shift(from_right, -1)
        mine[z_count - hop], mine[hop] = from_left, from_right
        other[z_count - hop], other[hop] = sibling(from_left), sibling(from_right)
    half = x.shape[0] // 2
    top, bottom = shift(from_left[:half], 1), shift(from_right[half:], -1)
    mine[middle] = jnp.concatenate([top, bottom], axis=0)
    other[middle] = jnp.concatenate([sibling(top), sibling(bottom)], axis=0)
    return mine, other


def across_rows(x):
    count = lax.axis_size("row")
    return [x] + [
        lax.ppermute(x, "row", [(r, r ^ d) for r in range(count)]) for d in range(1, count)
    ]


def on_device(factors):
    members = factors.shape[0]
    return jnp.stack([one_factor(factors[m]) for m in range(members)])


def one_factor(factor):
    rows_dev, cols_dev = factor.shape
    col_count, row_count = lax.axis_size("col"), lax.axis_size("row")
    z_count = col_count // 2
    order = rows_dev * row_count
    row_id, col_id = lax.axis_index("row"), lax.axis_index("col")
    z_id, core = col_id // 2, col_id % 2
    bpr = rows_dev // cols_dev
    slab = P_SIZE // col_count
    width = STEPS * slab
    total = STEPS * P_SIZE
    blocks = total // TILE
    direct = width == TILE and total == cols_dev and (row_count, z_count, bpr) == (4, 4, 2)
    if direct:
        factor3 = factor.reshape(bpr, cols_dev, cols_dev)
        part, ar, _, high, low = gather_factor(factor3, order, row_count, col_count)
        return apply_last(part, ar, high, low)
    row_global = row_id * rows_dev + jnp.arange(rows_dev, dtype=jnp.int32)
    col_global = col_id * cols_dev + jnp.arange(cols_dev, dtype=jnp.int32)
    on_diagonal = row_global[:, None] == col_global[None, :]
    local_trace = jnp.sum(jnp.where(on_diagonal, factor, 0.0))

    cols = factor[:, :width]
    rows = factor.reshape(bpr, cols_dev, cols_dev)[:, :width, :]
    diag = rows[:, :, :width].reshape(bpr * width, width)
    piece = jnp.concatenate([diag, jnp.full((8, width), local_trace)], axis=0)
    slabs = jnp.stack(across_rows(piece))
    mine, other = ring_rest(slabs, ring_first(slabs))
    gathered = jnp.stack([jnp.stack(mine), jnp.stack(other)])
    gathered, cols, rows = lax.optimization_barrier((gathered, cols, rows))

    first = ring_first(cols)
    row_pieces = across_rows(rows.reshape(bpr * width, cols_dev))
    at = jnp.stack([row_id, z_id, core]).astype(jnp.int32)
    square = jax.ShapeDtypeStruct((total, total), jnp.float32)
    params = pltpu.CompilerParams(vmem_limit_bytes=40 * 1024 * 1024)
    part, low = pl.pallas_call(
        functools.partial(place_kernel, 0, blocks // 2, bpr, slab, order),
        out_shape=(square, square),
        in_specs=[in_smem] + in_vmem(1),
        out_specs=tuple(in_vmem(2)),
        compiler_params=params,
        cost_estimate=cost(30_000_000_000),
    )(at, gathered)
    part, low, first = lax.optimization_barrier((part, low, first))
    mine, other = ring_rest(cols, first)
    inv, own = pl.pallas_call(
        functools.partial(finish_kernel, blocks // 2, blocks, bpr, slab, col_count),
        out_shape=(
            jax.ShapeDtypeStruct((col_count, total, width), jnp.float32),
            jax.ShapeDtypeStruct((bpr, width, width), jnp.float32),
        ),
        in_specs=[in_smem] + in_vmem(2),
        out_specs=tuple(in_vmem(2)),
        scratch_shapes=[pltpu.VMEM((total, total), jnp.float32)] * 2,
        compiler_params=params,
        cost_estimate=cost(25_000_000_000),
    )(at, part, low)
    damping = damping_share * jnp.sum(gathered[:, :, :, bpr * width, 0]) / order

    inv_rows = [
        lax.dynamic_index_in_dim(inv, (row_id ^ d) * bpr + b, 0, keepdims=False)
        for d in range(row_count)
        for b in range(bpr)
    ]
    inv_cols = [
        lax.dynamic_index_in_dim(
            inv, (z_id + z) % z_count * 2 + (core ^ side), 0, keepdims=False
        )
        for side in range(2)
        for z in range(z_count)
    ]
    cross = dot(
        jnp.concatenate(inv_rows, axis=1), jnp.concatenate(row_pieces, axis=0), ((1,), (0,))
    )
    lower = dot(
        jnp.concatenate(mine + other, axis=1), jnp.concatenate(inv_cols, axis=1), ((1,), (1,))
    )
    update = dot(lower, cross, ((1,), (0,)), three_pass)

    lower5 = lower.reshape(rows_dev, STEPS, col_count, slab)
    new_cols = lax.dynamic_index_in_dim(lower5, col_id, 2, keepdims=False)
    new_cols = new_cols.reshape(bpr, cols_dev, width)
    new_cols = new_cols.at[:, :width, :].set(own).reshape(rows_dev, width)

    trailing = (row_global % cols_dev >= width)[:, None] & (col_global % cols_dev >= width)[None, :]
    working = factor + jnp.where(on_diagonal, damping, 0.0)
    out = jnp.where(trailing, working - update, 0.0)
    return out.at[:, :width].set(new_cols)


def solution(mesh):
    placed = (P(None, "row", "col"),)
    return jax.shard_map(
        on_device, mesh=mesh, in_specs=placed, out_specs=P(None, "row", "col"), check_vma=False
    )
```
